32 devices in a mesh: img: 2 (over y), sub: 4 (over z), rng: 4 (over x, core).
Axes of the slice: x: 2, y: 2, z: 4, core: 2. Of those that a mesh axis runs over, the one named last changes fastest.
Arguments:
- image: bfloat16 [2, 16, 128, 4096], P(None, ('img', 'sub'), None, 'rng'), parts along dimension 1, may hold values from -6 to 6
- interp_weights: bfloat16 [4, 2, 2, 2, 128, 128], replicated, may hold values from -0.25 to 0.25
- range_taps: float32 [4, 4], replicated, may hold values from -2 to 2
- range_shifts: int32 [4, 2, 128], replicated, may hold values from -8 to 5
Outputs:
- merged_image: bfloat16 [2, 16, 128, 4096], P(None, ('img', 'sub'), None, 'rng'), parts along dimension 1
The draws below stay inside these ranges and needn't reach their ends.
There are 2 independent parts, one for each index of `img`. The reference program is written for one: setup_inputs(seed, part) draws one part's arguments, and reference() takes and returns one part's arrays. A program takes and returns all parts, laid end to end along the dimension named above; an argument that names none is the same for every part. Nothing has to cross between parts.
All inputs are finite; a program needn't handle non-finite values.
Results may differ from the reference program's by a relative error of at most 0.0095.
Values may be sent and summed in bfloat16 or wider, within the bound.
A program may use at most 64 MiB of HBM per device.

```python
import math
import jax
import jax.numpy as jnp
import numpy as np

ANGLES = 128
RANGE = 4096
RIM = 8
TAPS = 4
LEVELS = 4
GROUPS = 2
SUBIMAGES = 8
N_SUB = 4


def touch_ends(entries, rng, smallest, top_value):
    spot = [jax.random.randint(jax.random.fold_in(rng, axis), (), 0, length) for axis, length in enumerate(entries.shape)]
    widest = entries.shape.index(max(entries.shape))
    next_to = spot[:widest] + [(spot[widest] + 1) % entries.shape[widest]] + spot[widest + 1:]
    return entries.at[tuple(spot)].set(smallest).at[tuple(next_to)].set(top_value)


def block_levels(own_key, dims, cuts, least, high):
    gain, own = 1.0, jax.random.fold_in(own_key, 6)
    for dim, shards_of in cuts:
        draws = jnp.exp(jax.random.uniform(jax.random.fold_in(own, dim), (shards_of,), jnp.float32, least / len(cuts), high / len(cuts)))
        gain = gain * jnp.repeat(draws, dims[dim] // shards_of).reshape([-1 if axis == dim else 1 for axis in range(len(dims))])
    return gain


def normal_values(stream_key, shape, deviation, bound, cuts=(), held_as=jnp.bfloat16):
    entries = deviation * jax.random.normal(stream_key, shape, jnp.float32)
    if cuts:
        entries = entries * block_levels(stream_key, shape, cuts, -0.22, 0.18)
    return jnp.clip(entries, -bound, bound).astype(held_as)


def setup_inputs(seed: int = 0, part: int = 0) -> dict:
    streams_of = jax.random.split(jax.random.key(seed), 5)
    part_keys = jax.random.split(jax.random.fold_in(streams_of[4], part), 5)
    image = normal_values(part_keys[0], (2, SUBIMAGES, ANGLES, RANGE), 1.0, 6.0, ((1, 4), (3, 4)))
    interp_weights = normal_values(streams_of[1], (LEVELS, 2, 2, 2, ANGLES, ANGLES), (4 * ANGLES) ** -0.5, 0.25)
    range_taps = normal_values(streams_of[2], (LEVELS, TAPS), 0.5, 2.0, (), jnp.float32)
    range_shifts = touch_ends(jax.random.randint(streams_of[3], (LEVELS, 2, ANGLES), 0 - RIM, RIM - TAPS + 2), jax.random.fold_in(streams_of[3], 1), 0 - RIM, (RIM - TAPS + 2) - 1).astype(jnp.int32)
    return dict(image=image, interp_weights=interp_weights, range_taps=range_taps, range_shifts=range_shifts)


phase_step = 2.0 * math.pi / 64.0


def rotate(merged_sum, level_index, half_index, range_start, range_width):
    angle_rows = half_index * ANGLES + jnp.arange(ANGLES, dtype=jnp.int32)
    range_cols = range_start + jnp.arange(range_width, dtype=jnp.int32)
    wrapped = (range_cols[None, :] * (angle_rows[:, None] + 1) * (7 + level_index)) % 64
    phase = wrapped.astype(jnp.float32) * phase_step
    cosine = jnp.cos(phase)
    sinus = jnp.sin(phase)
    return jnp.stack([merged_sum[0] * cosine - merged_sum[1] * sinus, merged_sum[0] * sinus + merged_sum[1] * cosine])


def reference(image, interp_weights, range_taps, range_shifts):
    bit_count = N_SUB.bit_length() - 1
    count = N_SUB * GROUPS
    current = image
    for level_index in range(LEVELS):
        bit = level_index % bit_count
        stride = 2 ** bit
        side_of_rows = (np.arange(count) // GROUPS // stride) % 2
        padded = jnp.pad(current, ((0, 0), (0, 0), (0, 0), (RIM, RIM)))
        shift_rows = range_shifts[level_index][side_of_rows]
        base_index = (RIM + shift_rows[:, :, None] + jnp.arange(RANGE, dtype=jnp.int32)[None, None, :]).astype(jnp.int32)
        total = jnp.zeros(current.shape, jnp.float32)
        for tap_index in range(TAPS):
            gathered = jnp.stack([jnp.take_along_axis(padded[channel], base_index + tap_index, axis=2) for channel in range(2)])
            total = total + range_taps[level_index, tap_index] * gathered.astype(jnp.float32)
        interpolated = total.astype(jnp.bfloat16)
        split_rows = interpolated.reshape(2, N_SUB // (2 * stride), 2, stride, GROUPS, ANGLES, RANGE)
        half_images = []
        for half_index in range(2):
            merged_sum = jnp.zeros((2, N_SUB // (2 * stride), stride, GROUPS, ANGLES, RANGE), jnp.float32)
            for side_index in range(2):
                weight_pair = interp_weights[level_index, side_index, half_index].astype(jnp.float32)
                block_matrix = jnp.stack([jnp.stack([weight_pair[0], -weight_pair[1]]), jnp.stack([weight_pair[1], weight_pair[0]])])
                source = split_rows[:, :, side_index].astype(jnp.float32)
                merged_sum = merged_sum + jnp.einsum('xcij,chmgjr->xhmgir', block_matrix, source)
            half_images.append(rotate(merged_sum, level_index, half_index, 0, RANGE))
        current = jnp.stack(half_images, axis=2).reshape(2, count, ANGLES, RANGE).astype(jnp.bfloat16)
    return current
```

```python
import math

import functools

import jax
import jax.numpy as jnp
import numpy as np
from jax import lax
from jax.experimental import pallas as pl
from jax.experimental.pallas import tpu as pltpu
from jax.sharding import PartitionSpec as P

ANGLES = 128
RANGE = 4096
RIM = 8
TAPS = 4
LEVELS = 4


phase_step = 2.0 * math.pi / 64.0


def padded_2(cells, sides, width):
    for axis, dim in sides:
        count = lax.axis_size(axis)
        ends = count - 1
        head = lax.slice_in_dim(cells, 0, width, axis=dim)
        tail = lax.slice_in_dim(cells, cells.shape[dim] - width, cells.shape[dim], axis=dim)
        cells = jnp.concatenate(
            [
                lax.ppermute(tail, axis, [(i, (i + 1) % count) for i in range(ends)]),
                cells,
                lax.ppermute(head, axis, [((i + 1) % count, i) for i in range(ends)]),
            ],
            axis=dim,
        )
    return cells


def from_partner(value, axis, stride):
    mask = 2**stride
    pairs = [(source, source ^ mask) for source in range(lax.axis_size(axis))]
    return lax.ppermute(value, axis, pairs)


def rotate(merged_sum, level_index, half_index, range_start, range_width):
    angle_rows = half_index * ANGLES + jnp.arange(ANGLES, dtype=jnp.int32)
    range_cols = range_start + jnp.arange(range_width, dtype=jnp.int32)
    wrapped = range_cols[None, :] * (angle_rows[:, None] + 1) * (7 + level_index) % 64
    phase = wrapped.astype(jnp.float32) * phase_step
    cosine = jnp.cos(phase)
    sinus = jnp.sin(phase)
    return jnp.stack(
        [
            merged_sum[0] * cosine - merged_sum[1] * sinus,
            merged_sum[0] * sinus + merged_sum[1] * cosine,
        ]
    )


def level_coef(range_taps, range_shifts, level_index, side_index):
    offsets = jnp.arange(2 * RIM + 1, dtype=jnp.int32) - RIM
    tap_ids = jnp.arange(TAPS, dtype=jnp.int32)
    hits = (
        range_shifts[level_index, side_index][:, None, None] + tap_ids[None, :, None]
        == offsets[None, None, :]
    )
    return jnp.einsum(
        "t,ato->ao",
        range_taps[level_index],
        hits.astype(jnp.float32),
        precision=lax.Precision.HIGHEST,
    )


def interpolate(padded, coef, range_width):
    total = None
    for offset_index in range(2 * RIM + 1):
        term = coef[:, offset_index, None] * padded[
            ..., offset_index : offset_index + range_width
        ].astype(jnp.float32)
        total = term if total is None else total + term
    return total.astype(jnp.bfloat16)


def block_of(weight_pair):
    return jnp.stack(
        [jnp.stack([weight_pair[0], -weight_pair[1]]), jnp.stack([weight_pair[1], weight_pair[0]])]
    )


def combine_sides(lower_rows, upper_rows, weights_level, half_index):
    chosen = lax.dynamic_index_in_dim(weights_level, half_index, 1, keepdims=False)
    merged_sum = None
    for side_index, source in ((0, lower_rows), (1, upper_rows)):
        product = jnp.einsum(
            "xcij,cgjr->xgir",
            block_of(chosen[side_index]),
            source,
            preferred_element_type=jnp.float32,
        )
        merged_sum = product if merged_sum is None else merged_sum + product
    return merged_sum


def on_device(image, interp_weights, range_taps, range_shifts):
    range_width = image.shape[3]
    sub_count = lax.axis_size("sub")
    bit_count = sub_count.bit_length() - 1
    sub_index = lax.axis_index("sub")
    range_start = lax.axis_index("rng") * range_width
    current = padded_2(image, (("rng", 3),), LEVELS * RIM)
    margin = LEVELS * RIM
    for level_index in range(LEVELS):
        bit = level_index % bit_count
        own_half = sub_index // 2**bit % 2
        padded = current
        margin = margin - RIM
        out_width = range_width + 2 * margin
        coef = jnp.where(
            own_half == 0,
            level_coef(range_taps, range_shifts, level_index, 0),
            level_coef(range_taps, range_shifts, level_index, 1),
        )
        own_rows = interpolate(padded, coef, out_width)
        partner = from_partner(own_rows, "sub", bit)
        lower_rows = jnp.where(own_half == 0, own_rows, partner)
        upper_rows = jnp.where(own_half == 0, partner, own_rows)
        merged = combine_sides(lower_rows, upper_rows, interp_weights[level_index], own_half)
        turned = rotate(merged, level_index, own_half, range_start - margin, out_width)
        global_cols = range_start - margin + jnp.arange(out_width, dtype=jnp.int32)
        inside = jnp.logical_and(global_cols >= 0, global_cols < RANGE)
        turned = jnp.where(inside, turned, 0.0)
        current = turned.astype(jnp.bfloat16)
    return current


PERIOD = 64
LANES = 128
HALO = LEVELS * RIM
MESH = pl.DeviceIdType.MESH
NT = (((1,), (1,)), ((), ()))


def phase_tables():
    a = np.arange(ANGLES)
    tables = np.zeros((LEVELS, 2, 2, PERIOD, ANGLES), np.float32)
    for level in range(LEVELS):
        for half in range(2):
            start = -HALO if level < LEVELS - 1 else 0
            r = (start + np.arange(PERIOD))[:, None]
            wrapped = (r * (half * ANGLES + a + 1)[None, :] * (7 + level)) % PERIOD
            phase = wrapped * phase_step
            tables[level, half, 0] = np.cos(phase)
            tables[level, half, 1] = np.sin(phase)
    last = np.swapaxes(tables[LEVELS - 1], -1, -2)
    last = np.concatenate([last] * (LANES // PERIOD), -1)
    return tables[: LEVELS - 1], last


def merge_kernel(
    n, rngs, image_hbm, weights_hbm, taps, shifts, rows_hbm, cols_hbm, out,
    image, weights, rows_table, cols_table, load_sem,
    xt, xin, big, table, xf, sh0, sh1, sh2, ybuf, stage,
    in_send, in_recv, left_send, left_recv, right_send, right_recv, twin_send, twin_recv, out_send, out_recv,
):
    me = lax.axis_index("sub")
    place = lax.axis_index("rng")
    groups, width = image_hbm.shape[1], image_hbm.shape[3]
    block = width // n
    rows = block + 2 * HALO
    bits = n.bit_length() - 1

    twin = place % 2
    first = place - twin
    mine = 2 * me + twin
    near = (HALO, 0), (0, HALO)

    def span(b):
        start = b % n * block
        lo = max(start - near[b % 2][0], 0)
        hi = min(start + block + near[b % 2][1], width)
        return lo, HALO + lo - start, hi - lo

    def in_copy(g, src, b):
        lo, off, size = span(b)
        return pltpu.make_async_remote_copy(
            src_ref=xt.at[g, :, pl.ds(lo, size), :],
            dst_ref=xin.at[g, src, :, pl.ds(off, size), :],
            send_sem=in_send.at[g, b],
            recv_sem=in_recv.at[g, src],
            device_id={"sub": b // 2, "rng": first + b % 2},
            device_id_type=MESH,
        )

    def twin_copy(g, size_from, size_to):
        return pltpu.make_async_remote_copy(
            src_ref=xin.at[g, :, :, pl.ds(size_from, HALO), :],
            dst_ref=xin.at[g, :, :, pl.ds(size_to, HALO), :],
            send_sem=twin_send.at[g],
            recv_sem=twin_recv.at[g],
            device_id={"rng": place + 1 - 2 * twin},
            device_id_type=MESH,
        )

    def left_copy(g, src):
        return pltpu.make_async_remote_copy(
            src_ref=xt.at[g, :, pl.ds(width - HALO, HALO), :],
            dst_ref=xin.at[g, src, :, pl.ds(0, HALO), :],
            send_sem=left_send.at[g],
            recv_sem=left_recv.at[g, src],
            device_id={"sub": (1 - twin) * (n // 2), "rng": first + 2 * twin},
            device_id_type=MESH,
        )

    def right_copy(g, src):
        return pltpu.make_async_remote_copy(
            src_ref=xt.at[g, :, pl.ds(0, HALO), :],
            dst_ref=xin.at[g, src, :, pl.ds(rows - HALO, HALO), :],
            send_sem=right_send.at[g],
            recv_sem=right_recv.at[g, src],
            device_id={"sub": twin * (n // 2) + (1 - twin) * n - 1, "rng": first - 1 + 2 * twin},
            device_id_type=MESH,
        )

    def out_copy(g, z, owner):
        return pltpu.make_async_remote_copy(
            src_ref=stage.at[g, z],
            dst_ref=out.at[:, g, :, pl.ds(pl.multiple_of(owner % n * block, LANES), block)],
            send_sem=out_send.at[g, z],
            recv_sem=out_recv.at[g, owner % n],
            device_id={"sub": z, "rng": first + owner // n},
            device_id_type=MESH,
        )

    left_self = jnp.logical_and(twin == 0, me == n // 2)
    left_out = jnp.logical_and(jnp.logical_not(left_self), place < rngs - 1)
    right_self = jnp.logical_and(twin == 1, me == n // 2 - 1)
    right_out = jnp.logical_and(jnp.logical_not(right_self), place > 0)

    head_from_left = jnp.logical_and(mine == 0, place > 0)
    tail_from_right = jnp.logical_and(mine == 2 * n - 1, place < rngs - 1)
    barrier = pltpu.get_barrier_semaphore()

    def ready(cond, z, r):
        @pl.when(cond)
        def _():
            pl.semaphore_signal(
                barrier, inc=1, device_id={"sub": z, "rng": r}, device_id_type=MESH
            )

    for z in range(n):
        for c in range(2):
            ready(mine != 2 * z + c, z, first + c)
        ready(head_from_left, z, place - 1)
        ready(tail_from_right, z, place + 1)

    loads = [
        pltpu.make_async_copy(image_hbm.at[:, g], image.at[:, g], load_sem.at[g])
        for g in range(groups)
    ]
    others = [
        pltpu.make_async_copy(src, dst, load_sem.at[groups + k])
        for k, (src, dst) in enumerate(
            ((weights_hbm, weights), (rows_hbm, rows_table), (cols_hbm, cols_table))
        )
    ]
    for copy in loads + others:
        copy.start()

    eye = (
        lax.broadcasted_iota(jnp.int32, (LANES, LANES), 0)
        == lax.broadcasted_iota(jnp.int32, (LANES, LANES), 1)
    ).astype(jnp.bfloat16)

    for g in range(groups):
        loads[g].wait()
        for c in range(2):
            for k in range(width // LANES):
                cols = pl.ds(k * LANES, LANES)
                xt[g, c, cols, :] = lax.dot_general(
                    eye, image[c, g, :, cols], NT, preferred_element_type=jnp.float32
                ).astype(jnp.bfloat16)
        if g == 0:
            sends_edge = jnp.where(twin == 1, place < rngs - 1, place > 0)
            pl.semaphore_wait(barrier, 2 * n - 1 + sends_edge.astype(jnp.int32))

        @pl.when(left_out)
        def _():
            left_copy(g, me).start()

        @pl.when(right_out)
        def _():
            right_copy(g, me).start()

        for b in range(2 * n):

            @pl.when(jnp.logical_and(twin == b // n, mine != b))
            def _():
                in_copy(g, me, b).start()

    at_left = jnp.logical_and(place == 0, me == 0)
    at_right = jnp.logical_and(place == rngs - 1, me == n - 1)

    for b in range(2 * n):
        z = b // 2
        if b % 2 == b // n:

            @pl.when(mine == b)
            def _():
                lo, off, size = span(b)
                for g in range(groups):
                    xin[g, z, :, off : off + size, :] = xt[g, :, lo : lo + size, :]

    @pl.when(left_self)
    def _():
        for g in range(groups):
            xin[g, n // 2, :, :HALO, :] = xt[g, :, width - HALO :, :]

    @pl.when(right_self)
    def _():
        for g in range(groups):
            xin[g, n // 2 - 1, :, rows - HALO :, :] = xt[g, :, :HALO, :]

    @pl.when(at_left)
    def _():
        xin[:, :, :, :HALO, :] = jnp.zeros((groups, n, 2, HALO, ANGLES), jnp.bfloat16)

    @pl.when(at_right)
    def _():
        xin[:, :, :, rows - HALO :, :] = jnp.zeros((groups, n, 2, HALO, ANGLES), jnp.bfloat16)

    for copy in others:
        copy.wait()

    for level in range(LEVELS):
        for half in range(2):
            for side in range(2):
                real = weights[level, side, half, 0]
                imag = weights[level, side, half, 1]
                i = half * 2 * ANGLES
                j = side * 2 * ANGLES
                big[level, i : i + ANGLES, j : j + ANGLES] = real
                big[level, i : i + ANGLES, j + ANGLES : j + 2 * ANGLES] = -imag
                big[level, i + ANGLES : i + 2 * ANGLES, j : j + ANGLES] = imag
                big[level, i + ANGLES : i + 2 * ANGLES, j + ANGLES : j + 2 * ANGLES] = real
            if level < LEVELS - 1:
                for part in range(2):
                    for start in range(0, rows, PERIOD):
                        size = min(PERIOD, rows - start)
                        table[level, half, part, start : start + size, :] = rows_table[
                            level, half, part, :size, :
                        ]

    def send_back(g, s):
        here = jnp.logical_and(s == me, twin == mine // n)

        @pl.when(jnp.logical_not(here))
        def _():
            out_copy(g, s, mine).start()

        @pl.when(here)
        def _():
            out[:, g, :, pl.ds(pl.multiple_of(mine % n * block, LANES), block)] = stage[g, s]

    def per_group(g, carry):
        for b in range(2 * n):

            @pl.when(mine == b)
            def _():
                for src in range(n):
                    if b % 2 != b // n or src != b // 2:
                        in_copy(g, src, b).wait_recv()
                if b % 2 == 0:
                    twin_copy(g, block, 0).start()
                else:
                    twin_copy(g, HALO, rows - HALO).start()

        @pl.when(jnp.logical_or(mine == n, jnp.logical_and(mine == 0, place > 0)))
        def _():
            for src in range(n):

                @pl.when(jnp.logical_or(mine == 0, src != n // 2))
                def _():
                    left_copy(g, src).wait_recv()

        @pl.when(jnp.logical_or(mine == n - 1, jnp.logical_and(mine == 2 * n - 1, place < rngs - 1)))
        def _():
            for src in range(n):

                @pl.when(jnp.logical_or(mine == 2 * n - 1, src != n // 2 - 1))
                def _():
                    right_copy(g, src).wait_recv()

        twin_copy(g, 0, 0).wait()

        for s in range(n):
            for c in range(2):
                xf[s, c, :rows, :] = xin[g, s, c].astype(jnp.float32)

        for level in range(LEVELS):
            mask = 2 ** (level % bits)
            base = RIM * level
            count = rows - 2 * base
            kept = count - 2 * RIM
            wide = kept + RIM

            def per_pair(pair, inner, level=level, mask=mask, base=base, count=count, kept=kept, wide=wide):
                low = pair // mask * (2 * mask) + pair % mask
                members = (low, low + mask)
                for side in range(2):
                    k = shifts[level, side][None, :] + RIM
                    on8, on4, on2, on1 = [(k // p) % 2 == 1 for p in (8, 4, 2, 1)]
                    for c in range(2):
                        s = members[side]
                        u = None
                        for t in range(TAPS):
                            term = taps[level, t] * xf[s, c, pl.ds(base + t, count), :]
                            u = term if u is None else u + term
                        v = jnp.where(on8, u[RIM:], u[:wide])
                        sh0[:wide] = v
                        v = jnp.where(on4, sh0[pl.ds(4, wide), :], v)
                        sh1[:wide] = v
                        v = jnp.where(on2, sh1[pl.ds(2, wide), :], v)
                        sh2[:wide] = v
                        v = jnp.where(on1, sh2[pl.ds(1, kept), :], v[:kept])
                        j = (side * 2 + c) * ANGLES
                        ybuf[:kept, j : j + ANGLES] = v.astype(jnp.bfloat16)
                y = ybuf[:kept, :]
                if level < LEVELS - 1:
                    z = lax.dot_general(y, big[level], NT, preferred_element_type=jnp.float32)
                    for half in range(2):
                        s = members[half]
                        j = half * 2 * ANGLES
                        re, im = z[:, j : j + ANGLES], z[:, j + ANGLES : j + 2 * ANGLES]
                        span_rows = pl.ds(base + RIM, kept)
                        cosine = table[level, half, 0, span_rows, :]
                        sinus = table[level, half, 1, span_rows, :]
                        xf[s, 0, span_rows, :] = re * cosine - im * sinus
                        xf[s, 1, span_rows, :] = re * sinus + im * cosine
                else:
                    z = lax.dot_general(big[level], y, NT, preferred_element_type=jnp.float32)
                    for half in range(2):
                        s = members[half]
                        i = half * 2 * ANGLES
                        cosine, sinus = cols_table[half, 0], cols_table[half, 1]
                        for start in range(0, block, LANES):
                            cols = slice(start, start + LANES)
                            re, im = z[i : i + ANGLES, cols], z[i + ANGLES : i + 2 * ANGLES, cols]
                            stage[g, s, 0, :, cols] = (re * cosine - im * sinus).astype(jnp.bfloat16)
                            stage[g, s, 1, :, cols] = (re * sinus + im * cosine).astype(jnp.bfloat16)
                    for half in range(2):
                        send_back(g, members[half])

                return inner

            lax.fori_loop(0, n // 2, per_pair, 0)
            if level < LEVELS - 1:

                @pl.when(at_left)
                def _():
                    xf[:, :, :HALO, :] = jnp.zeros((n, 2, HALO, ANGLES), jnp.float32)

                @pl.when(at_right)
                def _():
                    xf[:, :, rows - HALO : rows, :] = jnp.zeros((n, 2, HALO, ANGLES), jnp.float32)

        return carry

    lax.fori_loop(0, groups, per_group, 0)

    for g in range(groups):
        for b in range(2 * n):

            @pl.when(jnp.logical_and(twin == b // n, mine != b))
            def _():
                in_copy(g, me, b).wait_send()

        for z in range(n):

            @pl.when(jnp.logical_not(jnp.logical_and(me == z, twin == mine // n)))
            def _():
                out_copy(g, z, mine).wait_send()

            @pl.when(mine != n * twin + z)
            def _():
                out_copy(g, z, n * twin + z).wait_recv()

        @pl.when(left_out)
        def _():
            left_copy(g, me).wait_send()

        @pl.when(right_out)
        def _():
            right_copy(g, me).wait_send()


def in_one_kernel(n, rngs, image, interp_weights, range_taps, range_shifts):
    groups, width = image.shape[1], image.shape[3]
    block = width // n
    rows = block + 2 * HALO
    rows_table, cols_table = phase_tables()
    vmem = pl.BlockSpec(memory_space=pltpu.VMEM)
    hbm = pl.BlockSpec(memory_space=pl.ANY)
    dma = pltpu.SemaphoreType.DMA
    f32, bf16 = jnp.float32, jnp.bfloat16
    return pl.pallas_call(
        functools.partial(merge_kernel, n, rngs),
        out_shape=pltpu.VMEM(image.shape, bf16),
        in_specs=[hbm, hbm, pl.BlockSpec(memory_space=pltpu.SMEM), vmem, hbm, hbm],
        out_specs=vmem,
        scratch_shapes=[
            pltpu.VMEM(image.shape, bf16),
            pltpu.VMEM(interp_weights.shape, bf16),
            pltpu.VMEM(rows_table.shape, f32),
            pltpu.VMEM(cols_table.shape, f32),
            dma((groups + 3,)),
            pltpu.VMEM((groups, 2, width, ANGLES), bf16),
            pltpu.VMEM((groups, n, 2, rows, ANGLES), bf16),
            pltpu.VMEM((LEVELS, 4 * ANGLES, 4 * ANGLES), bf16),
            pltpu.VMEM((LEVELS - 1, 2, 2, rows, ANGLES), f32),
            pltpu.VMEM((n, 2, rows + 8, ANGLES), f32),
            pltpu.VMEM((rows + 8, ANGLES), f32),
            pltpu.VMEM((rows + 8, ANGLES), f32),
            pltpu.VMEM((rows + 8, ANGLES), f32),
            pltpu.VMEM((rows, 4 * ANGLES), bf16),
            pltpu.VMEM((groups, n, 2, ANGLES, block), bf16),
            dma((groups, 2 * n)),
            dma((groups, n)),
            dma((groups,)),
            dma((groups, n)),
            dma((groups,)),
            dma((groups, n)),
            dma((groups,)),
            dma((groups,)),
            dma((groups, n)),
            dma((groups, n)),
        ],
        compiler_params=pltpu.CompilerParams(has_side_effects=True, collective_id=0),
    )(image, interp_weights, range_taps, range_shifts, rows_table, cols_table)


def fits_kernel(mesh, width):
    n = mesh.shape["sub"]
    block = width // n
    paired = mesh.shape["rng"] % 2 == 0
    return paired and n > 1 and n & (n - 1) == 0 and block % LANES == 0 and block >= HALO and ANGLES == LANES


def per_device(mesh, image, *rest):
    if fits_kernel(mesh, image.shape[3]):
        return in_one_kernel(mesh.shape["sub"], mesh.shape["rng"], image, *rest)
    return on_device(image, *rest)


def solution(mesh):
    return jax.shard_map(
        functools.partial(per_device, mesh),
        mesh=mesh,
        in_specs=(P(None, ("img", "sub"), None, "rng"), P(), P(), P()),
        out_specs=P(None, ("img", "sub"), None, "rng"),
        check_vma=False,
    )
```

```python
import math

import functools

import jax
import jax.numpy as jnp
import numpy as np
from jax import lax
from jax.experimental import pallas as pl
from jax.experimental.pallas import tpu as pltpu
from jax.sharding import PartitionSpec as P

ANGLES = 128
RANGE = 4096
RIM = 8
TAPS = 4
LEVELS = 4


phase_step = 2.0 * math.pi / 64.0


def padded_2(cells, sides, width):
    for axis, dim in sides:
        count = lax.axis_size(axis)
        ends = count - 1
        head = lax.slice_in_dim(cells, 0, width, axis=dim)
        tail = lax.slice_in_dim(cells, cells.shape[dim] - width, cells.shape[dim], axis=dim)
        cells = jnp.concatenate(
            [
                lax.ppermute(tail, axis, [(i, (i + 1) % count) for i in range(ends)]),
                cells,
                lax.ppermute(head, axis, [((i + 1) % count, i) for i in range(ends)]),
            ],
            axis=dim,
        )
    return cells


def from_partner(value, axis, stride):
    mask = 2**stride
    pairs = [(source, source ^ mask) for source in range(lax.axis_size(axis))]
    return lax.ppermute(value, axis, pairs)


def rotate(merged_sum, level_index, half_index, range_start, range_width):
    angle_rows = half_index * ANGLES + jnp.arange(ANGLES, dtype=jnp.int32)
    range_cols = range_start + jnp.arange(range_width, dtype=jnp.int32)
    wrapped = range_cols[None, :] * (angle_rows[:, None] + 1) * (7 + level_index) % 64
    phase = wrapped.astype(jnp.float32) * phase_step
    cosine = jnp.cos(phase)
    sinus = jnp.sin(phase)
    return jnp.stack(
        [
            merged_sum[0] * cosine - merged_sum[1] * sinus,
            merged_sum[0] * sinus + merged_sum[1] * cosine,
        ]
    )


def level_coef(range_taps, range_shifts, level_index, side_index):
    offsets = jnp.arange(2 * RIM + 1, dtype=jnp.int32) - RIM
    tap_ids = jnp.arange(TAPS, dtype=jnp.int32)
    hits = (
        range_shifts[level_index, side_index][:, None, None] + tap_ids[None, :, None]
        == offsets[None, None, :]
    )
    return jnp.einsum(
        "t,ato->ao",
        range_taps[level_index],
        hits.astype(jnp.float32),
        precision=lax.Precision.HIGHEST,
    )


def interpolate(padded, coef, range_width):
    total = None
    for offset_index in range(2 * RIM + 1):
        term = coef[:, offset_index, None] * padded[
            ..., offset_index : offset_index + range_width
        ].astype(jnp.float32)
        total = term if total is None else total + term
    return total.astype(jnp.bfloat16)


def block_of(weight_pair):
    return jnp.stack(
        [jnp.stack([weight_pair[0], -weight_pair[1]]), jnp.stack([weight_pair[1], weight_pair[0]])]
    )


def combine_sides(lower_rows, upper_rows, weights_level, half_index):
    chosen = lax.dynamic_index_in_dim(weights_level, half_index, 1, keepdims=False)
    merged_sum = None
    for side_index, source in ((0, lower_rows), (1, upper_rows)):
        product = jnp.einsum(
            "xcij,cgjr->xgir",
            block_of(chosen[side_index]),
            source,
            preferred_element_type=jnp.float32,
        )
        merged_sum = product if merged_sum is None else merged_sum + product
    return merged_sum


def on_device(image, interp_weights, range_taps, range_shifts):
    range_width = image.shape[3]
    sub_count = lax.axis_size("sub")
    bit_count = sub_count.bit_length() - 1
    sub_index = lax.axis_index("sub")
    range_start = lax.axis_index("rng") * range_width
    current = padded_2(image, (("rng", 3),), LEVELS * RIM)
    margin = LEVELS * RIM
    for level_index in range(LEVELS):
        bit = level_index % bit_count
        own_half = sub_index // 2**bit % 2
        padded = current
        margin = margin - RIM
        out_width = range_width + 2 * margin
        coef = jnp.where(
            own_half == 0,
            level_coef(range_taps, range_shifts, level_index, 0),
            level_coef(range_taps, range_shifts, level_index, 1),
        )
        own_rows = interpolate(padded, coef, out_width)
        partner = from_partner(own_rows, "sub", bit)
        lower_rows = jnp.where(own_half == 0, own_rows, partner)
        upper_rows = jnp.where(own_half == 0, partner, own_rows)
        merged = combine_sides(lower_rows, upper_rows, interp_weights[level_index], own_half)
        turned = rotate(merged, level_index, own_half, range_start - margin, out_width)
        global_cols = range_start - margin + jnp.arange(out_width, dtype=jnp.int32)
        inside = jnp.logical_and(global_cols >= 0, global_cols < RANGE)
        turned = jnp.where(inside, turned, 0.0)
        current = turned.astype(jnp.bfloat16)
    return current


PERIOD = 64
LANES = 128
CORES = 2
HALO = LEVELS * RIM
MESH = pl.DeviceIdType.MESH
NT = (((1,), (1,)), ((), ()))


def phase_tables():
    a = np.arange(ANGLES)
    tables = np.zeros((LEVELS, 2, 2, PERIOD, ANGLES), np.float32)
    for level in range(LEVELS):
        for half in range(2):
            start = -HALO if level < LEVELS - 1 else 0
            r = (start + np.arange(PERIOD))[:, None]
            wrapped = (r * (half * ANGLES + a + 1)[None, :] * (7 + level)) % PERIOD
            phase = wrapped * phase_step
            tables[level, half, 0] = np.cos(phase)
            tables[level, half, 1] = np.sin(phase)
    last = np.swapaxes(tables[LEVELS - 1], -1, -2)
    last = np.concatenate([last] * (LANES // PERIOD), -1)
    return tables[: LEVELS - 1], last


def merge_kernel(
    n, rngs, image_hbm, weights_hbm, taps, shifts, rows_hbm, cols_hbm, out,
    image, weights, rows_table, cols_table, load_sem,
    raw, xt, edges, halo, big, table, xf, sh0, sh1, sh2, ybuf, stage,
    tile_send, tile_recv, edge_send, edge_recv, twin_send, twin_recv, out_send, out_recv,
):
    me = lax.axis_index("sub")
    place = lax.axis_index("rng")
    width = image_hbm.shape[3]
    half_size = n // 2
    block = 2 * width // n
    tiles = block // LANES
    rows = LANES + 2 * HALO
    bits = n.bit_length() - 1

    twin = place % CORES
    first = place - twin
    mine = me // half_size
    spot = me % half_size
    at_left = jnp.logical_and(place == 0, spot == 0)
    at_right = jnp.logical_and(place == rngs - 1, spot == half_size - 1)

    def tile_of(core, j):
        return j + core * (tiles - 1 - 2 * j)

    def lanes(start):
        return pl.ds(pl.multiple_of(start, LANES), LANES)

    def tile_copy(m, core, j):
        return pltpu.make_async_remote_copy(
            src_ref=image.at[:, m, :, lanes(core * block + tile_of(core, j) * LANES)],
            dst_ref=raw.at[me, j],
            send_sem=tile_send.at[m, core, j],
            recv_sem=tile_recv.at[me, j],
            device_id={"sub": m * half_size + twin, "rng": first + core},
            device_id_type=MESH,
        )

    def tile_arrival(src, j):
        return pltpu.make_async_remote_copy(
            src_ref=raw.at[src, j],
            dst_ref=raw.at[src, j],
            send_sem=tile_send.at[0, 0, 0],
            recv_sem=tile_recv.at[src, j],
            device_id={"sub": src, "rng": first + spot},
            device_id_type=MESH,
        )

    def edge_home(side, m):
        return m * half_size + 1 - twin, first + 2 * twin - side

    def edge_copy(side, m, src):
        z, r = edge_home(side, m)
        return pltpu.make_async_remote_copy(
            src_ref=edges.at[side, m],
            dst_ref=halo.at[src],
            send_sem=edge_send.at[side, m],
            recv_sem=edge_recv.at[src],
            device_id={"sub": z, "rng": r},
            device_id_type=MESH,
        )

    def twin_copy():
        return pltpu.make_async_remote_copy(
            src_ref=xt.at[:, :, pl.ds(pl.multiple_of(block - twin * (block - HALO), HALO), HALO), :],
            dst_ref=xt.at[:, :, pl.ds(pl.multiple_of(twin * (block + HALO), HALO), HALO), :],
            send_sem=twin_send,
            recv_sem=twin_recv,
            device_id={"rng": place + 1 - 2 * twin},
            device_id_type=MESH,
        )

    def out_copy(j, z):
        return pltpu.make_async_remote_copy(
            src_ref=stage.at[j, z],
            dst_ref=out.at[:, mine, :, lanes(twin * block + tile_of(twin, j) * LANES)],
            send_sem=out_send.at[j, z],
            recv_sem=out_recv.at[mine, twin, j],
            device_id={"sub": z, "rng": first + spot},
            device_id_type=MESH,
        )

    def out_arrival(h, core, j):
        return pltpu.make_async_remote_copy(
            src_ref=stage.at[j, 0],
            dst_ref=out.at[:, h, :, lanes(core * block + tile_of(core, j) * LANES)],
            send_sem=out_send.at[0, 0],
            recv_sem=out_recv.at[h, core, j],
            device_id={"sub": h * half_size + twin, "rng": first + core},
            device_id_type=MESH,
        )

    def differs(z, r):
        return jnp.logical_or(me != z, place != r)

    barrier = pltpu.get_barrier_semaphore()

    def ready(cond, z, r):
        @pl.when(cond)
        def _():
            pl.semaphore_signal(
                barrier, inc=1, device_id={"sub": z, "rng": r}, device_id_type=MESH
            )

    head_from_left = jnp.logical_and(spot == 0, jnp.logical_and(twin == 0, place > 0))
    tail_from_right = jnp.logical_and(
        spot == half_size - 1, jnp.logical_and(twin == 1, place < rngs - 1)
    )
    for z in range(n):
        for c in range(CORES):
            ready(differs(z, first + c), z, first + c)
        ready(head_from_left, z, place - 1)
        ready(tail_from_right, z, place + 1)

    others = [
        pltpu.make_async_copy(src, dst, load_sem.at[2 + k])
        for k, (src, dst) in enumerate(
            ((weights_hbm, weights), (rows_hbm, rows_table), (cols_hbm, cols_table))
        )
    ]
    order = (1 - mine, mine)
    loads = [
        pltpu.make_async_copy(image_hbm.at[:, m], image.at[:, m], load_sem.at[k])
        for k, m in enumerate(order)
    ]
    for copy in loads + others:
        copy.start()

    goes_right = jnp.logical_or(twin == 0, place < rngs - 1)
    goes_left = jnp.logical_or(twin == 1, place > 0)
    leaves = jnp.where(twin == 1, place < rngs - 1, place > 0)
    pl.semaphore_wait(barrier, CORES * n - 1 + 2 * leaves.astype(jnp.int32))
    for copy in loads:
        copy.wait()

    def send_tiles(j):
        for core in range(CORES):
            tile_copy(1 - mine, core, j).start()
        for core in range(CORES):

            @pl.when(differs(mine * half_size + twin, first + core))
            def _():
                tile_copy(mine, core, j).start()

    send_tiles(0)

    def unit(count, shift):
        i = lax.broadcasted_iota(jnp.int32, (count, LANES), 0)
        k = lax.broadcasted_iota(jnp.int32, (count, LANES), 1)
        return (i + shift == k).astype(jnp.bfloat16)

    for side, (shift, start) in enumerate(((LANES - HALO, width - LANES), (0, 0))):
        pick = unit(HALO, shift)
        for m in range(2):
            for c in range(2):
                edges[side, m, c] = lax.dot_general(
                    pick, image[c, m, :, start : start + LANES], NT, preferred_element_type=jnp.float32
                ).astype(jnp.bfloat16)
            z, r = edge_home(side, m)
            exists = (goes_right, goes_left)[side]

            @pl.when(jnp.logical_and(exists, differs(z, r)))
            def _():
                edge_copy(side, m, me).start()

            @pl.when(jnp.logical_and(exists, jnp.logical_not(differs(z, r))))
            def _():
                halo[me] = edges[side, m]

    for j in range(1, tiles):
        send_tiles(j)

    for copy in others:
        copy.wait()

    for level in range(LEVELS):
        for half in range(2):
            for side in range(2):
                real = weights[level, side, half, 0]
                imag = weights[level, side, half, 1]
                i = half * 2 * ANGLES
                j = side * 2 * ANGLES
                big[level, i : i + ANGLES, j : j + ANGLES] = real
                big[level, i : i + ANGLES, j + ANGLES : j + 2 * ANGLES] = -imag
                big[level, i + ANGLES : i + 2 * ANGLES, j : j + ANGLES] = imag
                big[level, i + ANGLES : i + 2 * ANGLES, j + ANGLES : j + 2 * ANGLES] = real
            if level < LEVELS - 1:
                for part in range(2):
                    for start in range(0, rows, PERIOD):
                        size = min(PERIOD, rows - start)
                        table[level, half, part, start : start + size, :] = rows_table[
                            level, half, part, :size, :
                        ]

    eye = unit(LANES, 0)

    def take(j):
        at = HALO + tile_of(twin, j) * LANES

        @pl.when(twin == spot)
        def _():
            raw[me, j] = image[:, mine, :, lanes(twin * block + tile_of(twin, j) * LANES)]

        for src in range(n):

            @pl.when(differs(src, first + spot))
            def _():
                tile_arrival(src, j).wait_recv()

            for c in range(2):
                xt[src, c, pl.ds(pl.multiple_of(at, HALO), LANES), :] = lax.dot_general(
                    eye, raw[src, j, c], NT, preferred_element_type=jnp.float32
                )

    take(0)

    outer = jnp.logical_or(at_left, at_right)
    halo_at = pl.ds(pl.multiple_of(twin * (block + HALO), HALO), HALO)
    rim_at = pl.ds(pl.multiple_of(twin * (block + HALO), HALO), HALO)
    for src in range(n):
        gone = jnp.logical_and(spot != twin, src == me)

        @pl.when(jnp.logical_not(jnp.logical_or(outer, gone)))
        def _():
            edge_copy(0, 0, src).wait_recv()

    @pl.when(outer)
    def _():
        xt[:, :, halo_at, :] = jnp.zeros((n, 2, HALO, ANGLES), jnp.float32)

    @pl.when(jnp.logical_not(outer))
    def _():
        xt[:, :, rim_at, :] = halo[...].astype(jnp.float32)

    def send_back(j, s):
        here = jnp.logical_and(s == me, spot == twin)

        @pl.when(jnp.logical_not(here))
        def _():
            out_copy(j, s).start()

        @pl.when(here)
        def _():
            out[:, mine, :, lanes(twin * block + tile_of(twin, j) * LANES)] = stage[j, s]

    def per_tile(j, carry):
        @pl.when(j < tiles - 1)
        def _():
            take(j + 1)

        @pl.when(j == tiles - 2)
        def _():
            twin_copy().start()

        @pl.when(j == tiles - 1)
        def _():
            twin_copy().wait()

        start = pl.multiple_of(tile_of(twin, j) * LANES, LANES)

        for level in range(LEVELS):
            mask = 2 ** (level % bits)
            base = RIM * level
            count = rows - 2 * base
            kept = count - 2 * RIM
            wide = kept + RIM

            def per_pair(pair, inner, level=level, mask=mask, base=base, count=count, kept=kept, wide=wide):
                low = pair // mask * (2 * mask) + pair % mask
                members = (low, low + mask)
                for side in range(2):
                    k = shifts[level, side][None, :] + RIM
                    on8, on4, on2, on1 = [(k // p) % 2 == 1 for p in (8, 4, 2, 1)]
                    for c in range(2):
                        s = members[side]
                        held = xf.at[s, c] if level else xt.at[s, c, pl.ds(start, rows + 8)]
                        u = None
                        for t in range(TAPS):
                            term = taps[level, t] * held[pl.ds(base + t, count), :]
                            u = term if u is None else u + term
                        v = jnp.where(on8, u[RIM:], u[:wide])
                        sh0[:wide] = v
                        v = jnp.where(on4, sh0[pl.ds(4, wide), :], v)
                        sh1[:wide] = v
                        v = jnp.where(on2, sh1[pl.ds(2, wide), :], v)
                        sh2[:wide] = v
                        v = jnp.where(on1, sh2[pl.ds(1, kept), :], v[:kept])
                        i = (side * 2 + c) * ANGLES
                        ybuf[:kept, i : i + ANGLES] = v.astype(jnp.bfloat16)
                y = ybuf[:kept, :]
                if level < LEVELS - 1:
                    z = lax.dot_general(y, big[level], NT, preferred_element_type=jnp.float32)
                    for half in range(2):
                        s = members[half]
                        i = half * 2 * ANGLES
                        re, im = z[:, i : i + ANGLES], z[:, i + ANGLES : i + 2 * ANGLES]
                        span_rows = pl.ds(base + RIM, kept)
                        cosine = table[level, half, 0, span_rows, :]
                        sinus = table[level, half, 1, span_rows, :]
                        xf[s, 0, span_rows, :] = re * cosine - im * sinus
                        xf[s, 1, span_rows, :] = re * sinus + im * cosine
                else:
                    z = lax.dot_general(big[level], y, NT, preferred_element_type=jnp.float32)
                    for half in range(2):
                        s = members[half]
                        i = half * 2 * ANGLES
                        cosine, sinus = cols_table[half, 0], cols_table[half, 1]
                        re, im = z[i : i + ANGLES, :], z[i + ANGLES : i + 2 * ANGLES, :]
                        stage[j, s, 0] = (re * cosine - im * sinus).astype(jnp.bfloat16)
                        stage[j, s, 1] = (re * sinus + im * cosine).astype(jnp.bfloat16)
                    send_back(j, low + mask * (1 - mine))
                    send_back(j, low + mask * mine)

                return inner

            lax.fori_loop(0, n // 2, per_pair, 0)
            if level < LEVELS - 1:

                @pl.when(jnp.logical_and(at_left, j == 0))
                def _():
                    xf[:, :, :HALO, :] = jnp.zeros((n, 2, HALO, ANGLES), jnp.float32)

                @pl.when(jnp.logical_and(at_right, j == 0))
                def _():
                    xf[:, :, rows - HALO : rows, :] = jnp.zeros((n, 2, HALO, ANGLES), jnp.float32)

        return carry

    lax.fori_loop(0, tiles, per_tile, 0)

    for j in range(tiles):
        for core in range(CORES):
            tile_copy(1 - mine, core, j).wait_send()

            @pl.when(differs(mine * half_size + twin, first + core))
            def _():
                tile_copy(mine, core, j).wait_send()

    for side in range(2):
        for m in range(2):
            z, r = edge_home(side, m)

            @pl.when(jnp.logical_and((goes_right, goes_left)[side], differs(z, r)))
            def _():
                edge_copy(side, m, me).wait_send()

    for j in range(tiles):
        for z in range(n):

            @pl.when(differs(z, first + spot))
            def _():
                out_copy(j, z).wait_send()

        for h in range(2):
            for core in range(CORES):

                @pl.when(differs(h * half_size + twin, first + core))
                def _():
                    out_arrival(h, core, j).wait_recv()


def in_one_kernel(n, rngs, image, interp_weights, range_taps, range_shifts):
    width = image.shape[3]
    block = 2 * width // n
    tiles = block // LANES
    rows = LANES + 2 * HALO
    rows_table, cols_table = phase_tables()
    vmem = pl.BlockSpec(memory_space=pltpu.VMEM)
    hbm = pl.BlockSpec(memory_space=pl.ANY)
    dma = pltpu.SemaphoreType.DMA
    f32, bf16 = jnp.float32, jnp.bfloat16
    return pl.pallas_call(
        functools.partial(merge_kernel, n, rngs),
        out_shape=pltpu.VMEM(image.shape, bf16),
        in_specs=[hbm, hbm, pl.BlockSpec(memory_space=pltpu.SMEM), vmem, hbm, hbm],
        out_specs=vmem,
        scratch_shapes=[
            pltpu.VMEM(image.shape, bf16),
            pltpu.VMEM(interp_weights.shape, bf16),
            pltpu.VMEM(rows_table.shape, f32),
            pltpu.VMEM(cols_table.shape, f32),
            dma((5,)),
            pltpu.VMEM((n, tiles, 2, ANGLES, LANES), bf16),
            pltpu.VMEM((n, 2, block + 2 * HALO + 8, ANGLES), f32),
            pltpu.VMEM((2, 2, 2, HALO, ANGLES), bf16),
            pltpu.VMEM((n, 2, HALO, ANGLES), bf16),
            pltpu.VMEM((LEVELS, 4 * ANGLES, 4 * ANGLES), bf16),
            pltpu.VMEM((LEVELS - 1, 2, 2, rows, ANGLES), f32),
            pltpu.VMEM((n, 2, rows + 8, ANGLES), f32),
            pltpu.VMEM((rows + 8, ANGLES), f32),
            pltpu.VMEM((rows + 8, ANGLES), f32),
            pltpu.VMEM((rows + 8, ANGLES), f32),
            pltpu.VMEM((rows, 4 * ANGLES), bf16),
            pltpu.VMEM((tiles, n, 2, ANGLES, LANES), bf16),
            dma((2, CORES, tiles)),
            dma((n, tiles)),
            dma((2, 2)),
            dma((n,)),
            dma(()),
            dma(()),
            dma((tiles, n)),
            dma((2, CORES, tiles)),
        ],
        compiler_params=pltpu.CompilerParams(has_side_effects=True, collective_id=0),
    )(image, interp_weights, range_taps, range_shifts, rows_table, cols_table)


def fits_kernel(mesh, image_shape):
    n = mesh.shape["sub"]
    paired = mesh.shape["rng"] % CORES == 0
    tiled = image_shape[3] % (CORES * LANES) == 0 and image_shape[3] > CORES * LANES
    return paired and n == 2 * CORES and image_shape[1] == 2 and tiled and ANGLES == LANES


def per_device(mesh, image, *rest):
    if fits_kernel(mesh, image.shape):
        return in_one_kernel(mesh.shape["sub"], mesh.shape["rng"], image, *rest)
    return on_device(image, *rest)


def solution(mesh):
    return jax.shard_map(
        functools.partial(per_device, mesh),
        mesh=mesh,
        in_specs=(P(None, ("img", "sub"), None, "rng"), P(), P(), P()),
        out_specs=P(None, ("img", "sub"), None, "rng"),
        check_vma=False,
    )
```

```python
import math

import functools

import jax
import jax.numpy as jnp
import numpy as np
from jax import lax
from jax.experimental import pallas as pl
from jax.experimental.pallas import tpu as pltpu
from jax.sharding import PartitionSpec as P

ANGLES = 128
RANGE = 4096
RIM = 8
TAPS = 4
LEVELS = 4


phase_step = 2.0 * math.pi / 64.0


def padded_2(cells, sides, width):
    for axis, dim in sides:
        count = lax.axis_size(axis)
        ends = count - 1
        head = lax.slice_in_dim(cells, 0, width, axis=dim)
        tail = lax.slice_in_dim(cells, cells.shape[dim] - width, cells.shape[dim], axis=dim)
        cells = jnp.concatenate(
            [
                lax.ppermute(tail, axis, [(i, (i + 1) % count) for i in range(ends)]),
                cells,
                lax.ppermute(head, axis, [((i + 1) % count, i) for i in range(ends)]),
            ],
            axis=dim,
        )
    return cells


def from_partner(value, axis, stride):
    mask = 2**stride
    pairs = [(source, source ^ mask) for source in range(lax.axis_size(axis))]
    return lax.ppermute(value, axis, pairs)


def rotate(merged_sum, level_index, half_index, range_start, range_width):
    angle_rows = half_index * ANGLES + jnp.arange(ANGLES, dtype=jnp.int32)
    range_cols = range_start + jnp.arange(range_width, dtype=jnp.int32)
    wrapped = range_cols[None, :] * (angle_rows[:, None] + 1) * (7 + level_index) % 64
    phase = wrapped.astype(jnp.float32) * phase_step
    cosine = jnp.cos(phase)
    sinus = jnp.sin(phase)
    return jnp.stack(
        [
            merged_sum[0] * cosine - merged_sum[1] * sinus,
            merged_sum[0] * sinus + merged_sum[1] * cosine,
        ]
    )


def level_coef(range_taps, range_shifts, level_index, side_index):
    offsets = jnp.arange(2 * RIM + 1, dtype=jnp.int32) - RIM
    tap_ids = jnp.arange(TAPS, dtype=jnp.int32)
    hits = (
        range_shifts[level_index, side_index][:, None, None] + tap_ids[None, :, None]
        == offsets[None, None, :]
    )
    return jnp.einsum(
        "t,ato->ao",
        range_taps[level_index],
        hits.astype(jnp.float32),
        precision=lax.Precision.HIGHEST,
    )


def interpolate(padded, coef, range_width):
    total = None
    for offset_index in range(2 * RIM + 1):
        term = coef[:, offset_index, None] * padded[
            ..., offset_index : offset_index + range_width
        ].astype(jnp.float32)
        total = term if total is None else total + term
    return total.astype(jnp.bfloat16)


def block_of(weight_pair):
    return jnp.stack(
        [jnp.stack([weight_pair[0], -weight_pair[1]]), jnp.stack([weight_pair[1], weight_pair[0]])]
    )


def combine_sides(lower_rows, upper_rows, weights_level, half_index):
    chosen = lax.dynamic_index_in_dim(weights_level, half_index, 1, keepdims=False)
    merged_sum = None
    for side_index, source in ((0, lower_rows), (1, upper_rows)):
        product = jnp.einsum(
            "xcij,cgjr->xgir",
            block_of(chosen[side_index]),
            source,
            preferred_element_type=jnp.float32,
        )
        merged_sum = product if merged_sum is None else merged_sum + product
    return merged_sum


def on_device(image, interp_weights, range_taps, range_shifts):
    range_width = image.shape[3]
    sub_count = lax.axis_size("sub")
    bit_count = sub_count.bit_length() - 1
    sub_index = lax.axis_index("sub")
    range_start = lax.axis_index("rng") * range_width
    current = padded_2(image, (("rng", 3),), LEVELS * RIM)
    margin = LEVELS * RIM
    for level_index in range(LEVELS):
        bit = level_index % bit_count
        own_half = sub_index // 2**bit % 2
        padded = current
        margin = margin - RIM
        out_width = range_width + 2 * margin
        coef = jnp.where(
            own_half == 0,
            level_coef(range_taps, range_shifts, level_index, 0),
            level_coef(range_taps, range_shifts, level_index, 1),
        )
        own_rows = interpolate(padded, coef, out_width)
        partner = from_partner(own_rows, "sub", bit)
        lower_rows = jnp.where(own_half == 0, own_rows, partner)
        upper_rows = jnp.where(own_half == 0, partner, own_rows)
        merged = combine_sides(lower_rows, upper_rows, interp_weights[level_index], own_half)
        turned = rotate(merged, level_index, own_half, range_start - margin, out_width)
        global_cols = range_start - margin + jnp.arange(out_width, dtype=jnp.int32)
        inside = jnp.logical_and(global_cols >= 0, global_cols < RANGE)
        turned = jnp.where(inside, turned, 0.0)
        current = turned.astype(jnp.bfloat16)
    return current


PERIOD = 64
LANES = 128
CORES = 2
HALO = LEVELS * RIM
MESH = pl.DeviceIdType.MESH
NT = (((1,), (1,)), ((), ()))


def phase_tables():
    a = np.arange(ANGLES)
    tables = np.zeros((LEVELS, 2, 2, PERIOD, ANGLES), np.float32)
    for level in range(LEVELS):
        for half in range(2):
            start = -HALO if level < LEVELS - 1 else 0
            r = (start + np.arange(PERIOD))[:, None]
            wrapped = (r * (half * ANGLES + a + 1)[None, :] * (7 + level)) % PERIOD
            phase = wrapped * phase_step
            tables[level, half, 0] = np.cos(phase)
            tables[level, half, 1] = np.sin(phase)
    last = np.swapaxes(tables[LEVELS - 1], -1, -2)
    last = np.concatenate([last] * (LANES // PERIOD), -1)
    return tables[: LEVELS - 1], last


def merge_kernel(
    n, rngs, image_hbm, weights_hbm, taps_hbm, shifts_hbm, rows_hbm, cols_hbm, out,
    image, weights, taps, shifts, rows_table, cols_table, load_sem,
    raw, xt, edges, halo, big, table, xf, sh0, sh1, sh2, ybuf, stage,
    tile_send, tile_recv, edge_send, edge_recv, twin_send, twin_recv, out_send, out_recv,
    meet_send, meet_recv, seen, met,
):
    me = lax.axis_index("sub")
    place = lax.axis_index("rng")
    width = image_hbm.shape[3]
    half_size = n // 2
    block = 2 * width // n
    tiles = block // LANES
    rows = LANES + 2 * HALO
    bits = n.bit_length() - 1

    twin = place % CORES
    first = place - twin
    mine = me // half_size
    spot = me % half_size
    flip = place // CORES % 2
    home = twin + flip * (1 - 2 * twin)
    origin = spot + flip * (1 - 2 * spot)
    inner = twin != origin
    at_left = jnp.logical_and(place == 0, origin == 0)
    at_right = jnp.logical_and(place == rngs - 1, origin == CORES - 1)
    meets = jnp.logical_not(jnp.logical_or(inner, jnp.logical_or(at_left, at_right)))
    meets_right = jnp.logical_and(meets, twin == 1)
    meets_left = jnp.logical_and(meets, twin == 0)
    across = 1 - 2 * twin

    def tile_of(core, j):
        return j + core * (tiles - 1 - 2 * j)

    def lanes(start, count=1):
        return pl.ds(pl.multiple_of(start, LANES), count * LANES)

    def columns(core, j, count=1):
        return tile_of(core, j) * LANES - core * (count - 1) * LANES

    def part_copy(m, core, part):
        j, count = (0, 2) if part == 0 else (part + 1, 1)
        start = columns(core, j, count)
        return pltpu.make_async_remote_copy(
            src_ref=image.at[:, m, :, lanes(core * block + start, count)],
            dst_ref=raw.at[me, :, :, lanes(start, count)],
            send_sem=tile_send.at[m, core, part],
            recv_sem=tile_recv.at[me, part],
            device_id={"sub": m * half_size + home, "rng": first + core},
            device_id_type=MESH,
        )

    def part_arrival(src, part, count):
        here = raw.at[src, :, :, lanes(0, count)]
        return pltpu.make_async_remote_copy(
            src_ref=here,
            dst_ref=here,
            send_sem=tile_send.at[0, 0, 0],
            recv_sem=tile_recv.at[src, part],
            device_id={"sub": src, "rng": first + origin},
            device_id_type=MESH,
        )

    def edge_copy(m, src):
        return pltpu.make_async_remote_copy(
            src_ref=edges.at[m],
            dst_ref=halo.at[src],
            send_sem=edge_send.at[m],
            recv_sem=edge_recv.at[src],
            device_id={"sub": m * half_size + 1 - home},
            device_id_type=MESH,
        )

    def meet_copy():
        return pltpu.make_async_remote_copy(
            src_ref=xt.at[:, :, pl.ds(pl.multiple_of(HALO + twin * (block - HALO), HALO), HALO), :],
            dst_ref=xt.at[
                :, :, pl.ds(pl.multiple_of((1 - twin) * (block + HALO), HALO), HALO), :
            ],
            send_sem=meet_send,
            recv_sem=meet_recv,
            device_id={"rng": place - across},
            device_id_type=MESH,
        )

    def twin_copy():
        return pltpu.make_async_remote_copy(
            src_ref=xt.at[:, :, pl.ds(pl.multiple_of(block - twin * (block - HALO), HALO), HALO), :],
            dst_ref=xt.at[:, :, pl.ds(pl.multiple_of(twin * (block + HALO), HALO), HALO), :],
            send_sem=twin_send,
            recv_sem=twin_recv,
            device_id={"rng": place + 1 - 2 * twin},
            device_id_type=MESH,
        )

    def out_copy(j, count, z):
        start = columns(twin, j, count)
        return pltpu.make_async_remote_copy(
            src_ref=stage.at[z, :, :, lanes(start, count)],
            dst_ref=out.at[:, mine, :, lanes(twin * block + start, count)],
            send_sem=out_send.at[j, z],
            recv_sem=out_recv.at[mine, twin, j],
            device_id={"sub": z, "rng": first + origin},
            device_id_type=MESH,
        )

    def out_arrival(h, core, j, count):
        here = out.at[:, h, :, lanes(core * block + columns(core, j, count), count)]
        return pltpu.make_async_remote_copy(
            src_ref=here,
            dst_ref=here,
            send_sem=out_send.at[0, 0],
            recv_sem=out_recv.at[h, core, j],
            device_id={"sub": h * half_size + home, "rng": first + core},
            device_id_type=MESH,
        )

    def differs(z, r):
        return jnp.logical_or(me != z, place != r)

    def signal(sem, cond, z, r):
        @pl.when(cond)
        def _():
            pl.semaphore_signal(sem, inc=1, device_id={"sub": z, "rng": r}, device_id_type=MESH)

    def await_signal(sem, cond, count=1):
        @pl.when(cond)
        def _():
            pl.semaphore_wait(sem, count)

    barrier = pltpu.get_barrier_semaphore()
    for step in range(1, n):
        for c in range(CORES):
            signal(barrier, me + step < n, me + step, first + c)
    pl.semaphore_signal(
        barrier, inc=1, device_id={"rng": place + across}, device_id_type=MESH
    )
    signal(barrier, meets_right, me, place + 1)

    def load(k, m, start, size):
        cols = pl.ds(start, size)
        return pltpu.make_async_copy(image_hbm.at[:, m, :, cols], image.at[:, m, :, cols], load_sem.at[k])

    loads = [
        load(0, 1 - mine, 0, 2 * LANES),
        load(1, 1 - mine, width - 2 * LANES, 2 * LANES),
        load(2, mine, 0, width),
    ]
    if width > 4 * LANES:
        loads.append(load(3, 1 - mine, 2 * LANES, width - 4 * LANES))
    others = [
        pltpu.make_async_copy(src, dst, load_sem.at[4 + k])
        for k, (src, dst) in enumerate(
            (
                (weights_hbm, weights),
                (rows_hbm, rows_table),
                (cols_hbm, cols_table),
                (taps_hbm, taps),
                (shifts_hbm, shifts),
            )
        )
    ]
    for copy in loads + others:
        copy.start()

    def send_across(part):
        for core in range(CORES):
            part_copy(1 - mine, core, part).start()

    def send_along(part):
        for core in range(CORES):

            @pl.when(differs(mine * half_size + home, first + core))
            def _():
                part_copy(mine, core, part).start()

    pl.semaphore_wait(barrier, 1 + CORES * me + meets_left.astype(jnp.int32))
    for step in range(1, n):
        for c in range(CORES):
            signal(seen.at[step], me - step >= 0, me - step, first + c)
    signal(met, meets_left, me, place - 1)
    loads[0].wait()
    loads[1].wait()

    @pl.when(mine == 1)
    def _():
        send_across(0)

    loads[2].wait()

    @pl.when(home <= spot)
    def _():
        send_along(0)

    for copy in loads[3:]:
        copy.wait()
    for step in range(1, n):
        await_signal(seen.at[step], me + step < n, CORES)

        @pl.when(jnp.logical_and(mine == 0, half_size + home - me == step))
        def _():
            send_across(0)

        if step == 1:

            @pl.when(home > spot)
            def _():
                send_along(0)

    def unit(count, shift):
        i = lax.broadcasted_iota(jnp.int32, (count, LANES), 0)
        k = lax.broadcasted_iota(jnp.int32, (count, LANES), 1)
        return (i + shift == k).astype(jnp.bfloat16)

    pick = unit(HALO, (1 - twin) * (LANES - HALO))
    for m in range(2):
        for c in range(2):
            edges[m, c] = lax.dot_general(
                pick,
                image[c, m, :, lanes((1 - twin) * (width - LANES))],
                NT,
                preferred_element_type=jnp.float32,
            ).astype(jnp.bfloat16)

        @pl.when(m * half_size + 1 - home != me)
        def _():
            edge_copy(m, me).start()

        @pl.when(m * half_size + 1 - home == me)
        def _():
            halo[me] = edges[m]

    for part in range(1, tiles - 1):
        send_across(part)
        send_along(part)

    for copy in others:
        copy.wait()

    for level in range(LEVELS):
        for half in range(2):
            for side in range(2):
                real = weights[level, side, half, 0]
                imag = weights[level, side, half, 1]
                i = half * 2 * ANGLES
                j = side * 2 * ANGLES
                big[level, i : i + ANGLES, j : j + ANGLES] = real
                big[level, i : i + ANGLES, j + ANGLES : j + 2 * ANGLES] = -imag
                big[level, i + ANGLES : i + 2 * ANGLES, j : j + ANGLES] = imag
                big[level, i + ANGLES : i + 2 * ANGLES, j + ANGLES : j + 2 * ANGLES] = real
            if level < LEVELS - 1:
                for part in range(2):
                    for start in range(0, rows, PERIOD):
                        size = min(PERIOD, rows - start)
                        table[level, half, part, start : start + size, :] = rows_table[
                            level, half, part, :size, :
                        ]

    eye = unit(LANES, 0)

    @pl.when(twin == origin)
    def _():
        raw[me] = image[:, mine, :, lanes(twin * block, tiles)]

    def await_part(part, count):
        for src in range(n):

            @pl.when(differs(src, first + origin))
            def _():
                part_arrival(src, part, count).wait_recv()

    def take(j):
        start = tile_of(twin, j) * LANES
        for src in range(n):
            for c in range(2):
                xt[src, c, pl.ds(pl.multiple_of(HALO + start, HALO), LANES), :] = lax.dot_general(
                    eye, raw[src, c, :, lanes(start)], NT, preferred_element_type=jnp.float32
                )

    await_part(0, 2)
    take(0)

    await_signal(met, meets_right)
    halo_at = pl.ds(pl.multiple_of(twin * (block + HALO), HALO), HALO)

    @pl.when(meets)
    def _():
        meet_copy().start()
        meet_copy().wait()

    @pl.when(inner)
    def _():
        for src in range(n):

            @pl.when(src != me)
            def _():
                edge_copy(0, src).wait_recv()

        xt[:, :, halo_at, :] = halo[...].astype(jnp.float32)

    @pl.when(jnp.logical_or(at_left, at_right))
    def _():
        xt[:, :, halo_at, :] = jnp.zeros((n, 2, HALO, ANGLES), jnp.float32)

    def send_back(j, s):
        here = jnp.logical_and(s == me, origin == twin)

        @pl.when(jnp.logical_and(jnp.logical_not(here), j < tiles - 2))
        def _():
            out_copy(j, 1, s).start()

        @pl.when(jnp.logical_and(jnp.logical_not(here), j == tiles - 1))
        def _():
            out_copy(tiles - 2, 2, s).start()

        @pl.when(here)
        def _():
            cols = tile_of(twin, j) * LANES
            out[:, mine, :, lanes(twin * block + cols)] = stage[s, :, :, lanes(cols)]

    def per_tile(j, carry):
        @pl.when(jnp.logical_and(j > 0, j < tiles - 1))
        def _():
            await_part(j, 1)

        @pl.when(j < tiles - 1)
        def _():
            take(j + 1)

        @pl.when(j == tiles - 2)
        def _():
            twin_copy().start()

        @pl.when(j == tiles - 1)
        def _():
            twin_copy().wait()

        start = pl.multiple_of(tile_of(twin, j) * LANES, LANES)

        for level in range(LEVELS):
            mask = 2 ** (level % bits)
            base = RIM * level
            count = rows - 2 * base
            kept = count - 2 * RIM
            wide = kept + RIM

            def per_pair(pair, inner, level=level, mask=mask, base=base, count=count, kept=kept, wide=wide):
                low = pair // mask * (2 * mask) + pair % mask
                members = (low, low + mask)
                for side in range(2):
                    k = shifts[level, side][None, :] + RIM
                    on8, on4, on2, on1 = [(k // p) % 2 == 1 for p in (8, 4, 2, 1)]
                    for c in range(2):
                        s = members[side]
                        b = side * 2 + c
                        held = xf.at[s, c] if level else xt.at[s, c, pl.ds(start, rows + 8)]
                        u = None
                        for t in range(TAPS):
                            term = taps[level, t] * held[pl.ds(base + t, count), :]
                            u = term if u is None else u + term
                        v = jnp.where(on8, u[RIM:], u[:wide])
                        sh0[b, :wide] = v
                        v = jnp.where(on4, sh0[b, pl.ds(4, wide), :], v)
                        sh1[b, :wide] = v
                        v = jnp.where(on2, sh1[b, pl.ds(2, wide), :], v)
                        sh2[b, :wide] = v
                        v = jnp.where(on1, sh2[b, pl.ds(1, kept), :], v[:kept])
                        i = (side * 2 + c) * ANGLES
                        ybuf[pair, :kept, i : i + ANGLES] = v.astype(jnp.bfloat16)
                y = ybuf[pair, :kept, :]
                if level < LEVELS - 1:
                    z = lax.dot_general(y, big[level], NT, preferred_element_type=jnp.float32)
                    for half in range(2):
                        s = members[half]
                        i = half * 2 * ANGLES
                        re, im = z[:, i : i + ANGLES], z[:, i + ANGLES : i + 2 * ANGLES]
                        span_rows = pl.ds(base + RIM, kept)
                        cosine = table[level, half, 0, span_rows, :]
                        sinus = table[level, half, 1, span_rows, :]
                        xf[s, 0, span_rows, :] = re * cosine - im * sinus
                        xf[s, 1, span_rows, :] = re * sinus + im * cosine
                else:
                    z = lax.dot_general(big[level], y, NT, preferred_element_type=jnp.float32)
                    for half in range(2):
                        s = members[half]
                        i = half * 2 * ANGLES
                        cosine, sinus = cols_table[half, 0], cols_table[half, 1]
                        re, im = z[i : i + ANGLES, :], z[i + ANGLES : i + 2 * ANGLES, :]
                        stage[s, 0, :, lanes(start)] = (re * cosine - im * sinus).astype(jnp.bfloat16)
                        stage[s, 1, :, lanes(start)] = (re * sinus + im * cosine).astype(jnp.bfloat16)
                    send_back(j, low + mask * (1 - mine))
                    send_back(j, low + mask * mine)

                return inner

            for pair in range(n // 2):
                per_pair(pair, 0)
            if level < LEVELS - 1:

                @pl.when(jnp.logical_and(at_left, j == 0))
                def _():
                    xf[:, :, :HALO, :] = jnp.zeros((n, 2, HALO, ANGLES), jnp.float32)

                @pl.when(jnp.logical_and(at_right, j == 0))
                def _():
                    xf[:, :, rows - HALO : rows, :] = jnp.zeros((n, 2, HALO, ANGLES), jnp.float32)

        return carry

    lax.fori_loop(0, tiles, per_tile, 0)

    for part in range(tiles - 1):
        for core in range(CORES):
            part_copy(1 - mine, core, part).wait_send()

            @pl.when(differs(mine * half_size + home, first + core))
            def _():
                part_copy(mine, core, part).wait_send()

    for m in range(2):

        @pl.when(m * half_size + 1 - home != me)
        def _():
            edge_copy(m, me).wait_send()

    for j in range(tiles - 1):
        count = 1 + (j == tiles - 2)
        for z in range(n):

            @pl.when(differs(z, first + origin))
            def _():
                out_copy(j, count, z).wait_send()

        for h in range(2):
            for core in range(CORES):

                @pl.when(differs(h * half_size + home, first + core))
                def _():
                    out_arrival(h, core, j, count).wait_recv()


def in_one_kernel(n, rngs, image, interp_weights, range_taps, range_shifts):
    width = image.shape[3]
    block = 2 * width // n
    tiles = block // LANES
    rows = LANES + 2 * HALO
    rows_table, cols_table = phase_tables()
    vmem = pl.BlockSpec(memory_space=pltpu.VMEM)
    hbm = pl.BlockSpec(memory_space=pl.ANY)
    dma = pltpu.SemaphoreType.DMA
    f32, bf16 = jnp.float32, jnp.bfloat16
    return pl.pallas_call(
        functools.partial(merge_kernel, n, rngs),
        out_shape=pltpu.VMEM(image.shape, bf16),
        in_specs=[hbm] * 6,
        out_specs=vmem,
        scratch_shapes=[
            pltpu.VMEM(image.shape, bf16),
            pltpu.VMEM(interp_weights.shape, bf16),
            pltpu.SMEM(range_taps.shape, f32),
            pltpu.VMEM(range_shifts.shape, jnp.int32),
            pltpu.VMEM(rows_table.shape, f32),
            pltpu.VMEM(cols_table.shape, f32),
            dma((9,)),
            pltpu.VMEM((n, 2, ANGLES, block), bf16),
            pltpu.VMEM((n, 2, block + 2 * HALO + 8, ANGLES), f32),
            pltpu.VMEM((2, 2, HALO, ANGLES), bf16),
            pltpu.VMEM((n, 2, HALO, ANGLES), bf16),
            pltpu.VMEM((LEVELS, 4 * ANGLES, 4 * ANGLES), bf16),
            pltpu.VMEM((LEVELS - 1, 2, 2, rows, ANGLES), f32),
            pltpu.VMEM((n, 2, rows + 8, ANGLES), f32),
            pltpu.VMEM((4, rows + 8, ANGLES), f32),
            pltpu.VMEM((4, rows + 8, ANGLES), f32),
            pltpu.VMEM((4, rows + 8, ANGLES), f32),
            pltpu.VMEM((n // 2, rows, 4 * ANGLES), bf16),
            pltpu.VMEM((n, 2, ANGLES, block), bf16),
            dma((2, CORES, tiles - 1)),
            dma((n, tiles - 1)),
            dma((2,)),
            dma((n,)),
            dma(()),
            dma(()),
            dma((tiles - 1, n)),
            dma((2, CORES, tiles - 1)),
            dma(()),
            dma(()),
            pltpu.SemaphoreType.REGULAR((n,)),
            pltpu.SemaphoreType.REGULAR,
        ],
        compiler_params=pltpu.CompilerParams(has_side_effects=True, collective_id=0),
    )(image, interp_weights, range_taps, range_shifts, rows_table, cols_table)


def fits_kernel(mesh, image_shape):
    n = mesh.shape["sub"]
    paired = mesh.shape["rng"] % CORES == 0
    tiled = image_shape[3] % (CORES * LANES) == 0 and image_shape[3] > CORES * LANES
    return paired and n == 2 * CORES and image_shape[1] == 2 and tiled and ANGLES == LANES


def per_device(mesh, image, *rest):
    if fits_kernel(mesh, image.shape):
        return in_one_kernel(mesh.shape["sub"], mesh.shape["rng"], image, *rest)
    return on_device(image, *rest)


def solution(mesh):
    return jax.shard_map(
        functools.partial(per_device, mesh),
        mesh=mesh,
        in_specs=(P(None, ("img", "sub"), None, "rng"), P(), P(), P()),
        out_specs=P(None, ("img", "sub"), None, "rng"),
        check_vma=False,
    )
```

```python
import math

import functools

import jax
import jax.numpy as jnp
import numpy as np
from jax import lax
from jax.experimental import pallas as pl
from jax.experimental.pallas import tpu as pltpu
from jax.sharding import PartitionSpec as P

ANGLES = 128
RANGE = 4096
RIM = 8
TAPS = 4
LEVELS = 4


phase_step = 2.0 * math.pi / 64.0


def padded_2(cells, sides, width):
    for axis, dim in sides:
        count = lax.axis_size(axis)
        ends = count - 1
        head = lax.slice_in_dim(cells, 0, width, axis=dim)
        tail = lax.slice_in_dim(cells, cells.shape[dim] - width, cells.shape[dim], axis=dim)
        cells = jnp.concatenate(
            [
                lax.ppermute(tail, axis, [(i, (i + 1) % count) for i in range(ends)]),
                cells,
                lax.ppermute(head, axis, [((i + 1) % count, i) for i in range(ends)]),
            ],
            axis=dim,
        )
    return cells


def from_partner(value, axis, stride):
    mask = 2**stride
    pairs = [(source, source ^ mask) for source in range(lax.axis_size(axis))]
    return lax.ppermute(value, axis, pairs)


def rotate(merged_sum, level_index, half_index, range_start, range_width):
    angle_rows = half_index * ANGLES + jnp.arange(ANGLES, dtype=jnp.int32)
    range_cols = range_start + jnp.arange(range_width, dtype=jnp.int32)
    wrapped = range_cols[None, :] * (angle_rows[:, None] + 1) * (7 + level_index) % 64
    phase = wrapped.astype(jnp.float32) * phase_step
    cosine = jnp.cos(phase)
    sinus = jnp.sin(phase)
    return jnp.stack(
        [
            merged_sum[0] * cosine - merged_sum[1] * sinus,
            merged_sum[0] * sinus + merged_sum[1] * cosine,
        ]
    )


def level_coef(range_taps, range_shifts, level_index, side_index):
    offsets = jnp.arange(2 * RIM + 1, dtype=jnp.int32) - RIM
    tap_ids = jnp.arange(TAPS, dtype=jnp.int32)
    hits = (
        range_shifts[level_index, side_index][:, None, None] + tap_ids[None, :, None]
        == offsets[None, None, :]
    )
    return jnp.einsum(
        "t,ato->ao",
        range_taps[level_index],
        hits.astype(jnp.float32),
        precision=lax.Precision.HIGHEST,
    )


def interpolate(padded, coef, range_width):
    total = None
    for offset_index in range(2 * RIM + 1):
        term = coef[:, offset_index, None] * padded[
            ..., offset_index : offset_index + range_width
        ].astype(jnp.float32)
        total = term if total is None else total + term
    return total.astype(jnp.bfloat16)


def block_of(weight_pair):
    return jnp.stack(
        [jnp.stack([weight_pair[0], -weight_pair[1]]), jnp.stack([weight_pair[1], weight_pair[0]])]
    )


def combine_sides(lower_rows, upper_rows, weights_level, half_index):
    chosen = lax.dynamic_index_in_dim(weights_level, half_index, 1, keepdims=False)
    merged_sum = None
    for side_index, source in ((0, lower_rows), (1, upper_rows)):
        product = jnp.einsum(
            "xcij,cgjr->xgir",
            block_of(chosen[side_index]),
            source,
            preferred_element_type=jnp.float32,
        )
        merged_sum = product if merged_sum is None else merged_sum + product
    return merged_sum


def on_device(image, interp_weights, range_taps, range_shifts):
    range_width = image.shape[3]
    sub_count = lax.axis_size("sub")
    bit_count = sub_count.bit_length() - 1
    sub_index = lax.axis_index("sub")
    range_start = lax.axis_index("rng") * range_width
    current = padded_2(image, (("rng", 3),), LEVELS * RIM)
    margin = LEVELS * RIM
    for level_index in range(LEVELS):
        bit = level_index % bit_count
        own_half = sub_index // 2**bit % 2
        padded = current
        margin = margin - RIM
        out_width = range_width + 2 * margin
        coef = jnp.where(
            own_half == 0,
            level_coef(range_taps, range_shifts, level_index, 0),
            level_coef(range_taps, range_shifts, level_index, 1),
        )
        own_rows = interpolate(padded, coef, out_width)
        partner = from_partner(own_rows, "sub", bit)
        lower_rows = jnp.where(own_half == 0, own_rows, partner)
        upper_rows = jnp.where(own_half == 0, partner, own_rows)
        merged = combine_sides(lower_rows, upper_rows, interp_weights[level_index], own_half)
        turned = rotate(merged, level_index, own_half, range_start - margin, out_width)
        global_cols = range_start - margin + jnp.arange(out_width, dtype=jnp.int32)
        inside = jnp.logical_and(global_cols >= 0, global_cols < RANGE)
        turned = jnp.where(inside, turned, 0.0)
        current = turned.astype(jnp.bfloat16)
    return current


PERIOD = 64
LANES = 128
CORES = 2
HALO = LEVELS * RIM
MESH = pl.DeviceIdType.MESH
NT = (((1,), (1,)), ((), ()))


def phase_tables():
    a = np.arange(ANGLES)
    tables = np.zeros((LEVELS, 2, 2, PERIOD, ANGLES), np.float32)
    for level in range(LEVELS):
        for half in range(2):
            start = -HALO if level < LEVELS - 1 else 0
            r = (start + np.arange(PERIOD))[:, None]
            wrapped = (r * (half * ANGLES + a + 1)[None, :] * (7 + level)) % PERIOD
            phase = wrapped * phase_step
            tables[level, half, 0] = np.cos(phase)
            tables[level, half, 1] = np.sin(phase)
    last = np.swapaxes(tables[LEVELS - 1], -1, -2)
    last = np.concatenate([last] * (LANES // PERIOD), -1)
    return tables[: LEVELS - 1], last


def merge_kernel(
    n, rngs, image_hbm, weights_hbm, taps_hbm, shifts_hbm, rows_hbm, cols_hbm, out,
    image, weights, taps, shifts, rows_table, cols_table, load_sem,
    raw, xt, edges, halo, big, table, xf, sh0, sh1, sh2, ybuf, stage,
    tile_send, tile_recv, edge_send, edge_recv, twin_send, twin_recv, out_send, out_recv,
    meet_send, meet_recv, seen, met,
):
    me = lax.axis_index("sub")
    place = lax.axis_index("rng")
    width = image_hbm.shape[3]
    half_size = n // 2
    block = 2 * width // n
    tiles = block // LANES
    rows = LANES + 2 * HALO
    bits = n.bit_length() - 1

    twin = place % CORES
    first = place - twin
    mine = me // half_size
    spot = me % half_size
    flip = place // CORES % 2
    home = twin + flip * (1 - 2 * twin)
    origin = spot + flip * (1 - 2 * spot)
    inner = twin != origin
    at_left = jnp.logical_and(place == 0, origin == 0)
    at_right = jnp.logical_and(place == rngs - 1, origin == CORES - 1)
    meets = jnp.logical_not(jnp.logical_or(inner, jnp.logical_or(at_left, at_right)))
    meets_right = jnp.logical_and(meets, twin == 1)
    meets_left = jnp.logical_and(meets, twin == 0)
    across = 1 - 2 * twin

    def tile_of(core, j):
        return j + core * (tiles - 1 - 2 * j)

    def lanes(start, count=1):
        return pl.ds(pl.multiple_of(start, LANES), count * LANES)

    def columns(core, j, count=1):
        return tile_of(core, j) * LANES - core * (count - 1) * LANES

    def part_copy(m, core, part):
        j, count = (0, 2) if part == 0 else (part + 1, 1)
        start = columns(core, j, count)
        return pltpu.make_async_remote_copy(
            src_ref=image.at[:, m, :, lanes(core * block + start, count)],
            dst_ref=raw.at[me, :, :, lanes(start, count)],
            send_sem=tile_send.at[m, core, part],
            recv_sem=tile_recv.at[me, part],
            device_id={"sub": m * half_size + home, "rng": first + core},
            device_id_type=MESH,
        )

    def part_arrival(src, part, count):
        here = raw.at[src, :, :, lanes(0, count)]
        return pltpu.make_async_remote_copy(
            src_ref=here,
            dst_ref=here,
            send_sem=tile_send.at[0, 0, 0],
            recv_sem=tile_recv.at[src, part],
            device_id={"sub": src, "rng": first + origin},
            device_id_type=MESH,
        )

    def edge_copy(m, src):
        return pltpu.make_async_remote_copy(
            src_ref=edges.at[m],
            dst_ref=halo.at[src],
            send_sem=edge_send.at[m],
            recv_sem=edge_recv.at[src],
            device_id={"sub": m * half_size + 1 - home},
            device_id_type=MESH,
        )

    def meet_copy():
        return pltpu.make_async_remote_copy(
            src_ref=xt.at[:, :, pl.ds(pl.multiple_of(HALO + twin * (block - HALO), HALO), HALO), :],
            dst_ref=xt.at[
                :, :, pl.ds(pl.multiple_of((1 - twin) * (block + HALO), HALO), HALO), :
            ],
            send_sem=meet_send,
            recv_sem=meet_recv,
            device_id={"rng": place - across},
            device_id_type=MESH,
        )

    def twin_copy():
        return pltpu.make_async_remote_copy(
            src_ref=xt.at[:, :, pl.ds(pl.multiple_of(block - twin * (block - HALO), HALO), HALO), :],
            dst_ref=xt.at[:, :, pl.ds(pl.multiple_of(twin * (block + HALO), HALO), HALO), :],
            send_sem=twin_send,
            recv_sem=twin_recv,
            device_id={"rng": place + 1 - 2 * twin},
            device_id_type=MESH,
        )

    def out_copy(j, count, z):
        start = columns(twin, j, count)
        return pltpu.make_async_remote_copy(
            src_ref=stage.at[z, :, :, lanes(start, count)],
            dst_ref=out.at[:, mine, :, lanes(twin * block + start, count)],
            send_sem=out_send.at[j, z],
            recv_sem=out_recv.at[mine, twin, j],
            device_id={"sub": z, "rng": first + origin},
            device_id_type=MESH,
        )

    def out_arrival(h, core, j, count):
        here = out.at[:, h, :, lanes(core * block + columns(core, j, count), count)]
        return pltpu.make_async_remote_copy(
            src_ref=here,
            dst_ref=here,
            send_sem=out_send.at[0, 0],
            recv_sem=out_recv.at[h, core, j],
            device_id={"sub": h * half_size + home, "rng": first + core},
            device_id_type=MESH,
        )

    def differs(z, r):
        return jnp.logical_or(me != z, place != r)

    def signal(sem, cond, z, r):
        @pl.when(cond)
        def _():
            pl.semaphore_signal(sem, inc=1, device_id={"sub": z, "rng": r}, device_id_type=MESH)

    def await_signal(sem, cond, count=1):
        @pl.when(cond)
        def _():
            pl.semaphore_wait(sem, count)

    def load(k, m, start, size):
        cols = pl.ds(start, size)
        return pltpu.make_async_copy(image_hbm.at[:, m, :, cols], image.at[:, m, :, cols], load_sem.at[k])

    loads = [
        load(0, 1 - mine, 0, 2 * LANES),
        load(1, 1 - mine, width - 2 * LANES, 2 * LANES),
        load(2, mine, 0, width),
    ]
    if width > 4 * LANES:
        loads.append(load(3, 1 - mine, 2 * LANES, width - 4 * LANES))
    others = [
        pltpu.make_async_copy(src, dst, load_sem.at[4 + k])
        for k, (src, dst) in enumerate(
            (
                (weights_hbm, weights),
                (rows_hbm, rows_table),
                (cols_hbm, cols_table),
                (taps_hbm, taps),
                (shifts_hbm, shifts),
            )
        )
    ]
    for copy in loads + others:
        copy.start()

    barrier = pltpu.get_barrier_semaphore()
    for step in range(1, n):
        for c in range(CORES):
            signal(barrier, me + step < n, me + step, first + c)
    pl.semaphore_signal(
        barrier, inc=1, device_id={"rng": place + across}, device_id_type=MESH
    )
    signal(barrier, meets_right, me, place + 1)

    def send_across(part):
        for core in range(CORES):
            part_copy(1 - mine, core, part).start()

    def send_along(part):
        for core in range(CORES):

            @pl.when(differs(mine * half_size + home, first + core))
            def _():
                part_copy(mine, core, part).start()

    pl.semaphore_wait(barrier, 1 + CORES * me + meets_left.astype(jnp.int32))
    for step in range(1, n):
        for c in range(CORES):
            signal(seen.at[step], me - step >= 0, me - step, first + c)
    signal(met, meets_left, me, place - 1)
    loads[0].wait()
    loads[1].wait()

    @pl.when(mine == 1)
    def _():
        send_across(0)

    loads[2].wait()

    @pl.when(home <= spot)
    def _():
        send_along(0)

    for copy in loads[3:]:
        copy.wait()
    for step in range(1, n):
        await_signal(seen.at[step], me + step < n, CORES)

        @pl.when(jnp.logical_and(mine == 0, half_size + home - me == step))
        def _():
            send_across(0)

        if step == 1:

            @pl.when(home > spot)
            def _():
                send_along(0)

    def unit(count, shift):
        i = lax.broadcasted_iota(jnp.int32, (count, LANES), 0)
        k = lax.broadcasted_iota(jnp.int32, (count, LANES), 1)
        return (i + shift == k).astype(jnp.bfloat16)

    pick = unit(HALO, (1 - twin) * (LANES - HALO))
    for m in range(2):
        for c in range(2):
            edges[m, c] = lax.dot_general(
                pick,
                image[c, m, :, lanes((1 - twin) * (width - LANES))],
                NT,
                preferred_element_type=jnp.float32,
            ).astype(jnp.bfloat16)

        @pl.when(m * half_size + 1 - home != me)
        def _():
            edge_copy(m, me).start()

        @pl.when(m * half_size + 1 - home == me)
        def _():
            halo[me] = edges[m]

    for part in range(1, tiles - 1):
        send_across(part)
        send_along(part)

    for copy in others:
        copy.wait()

    for level in range(LEVELS):
        for half in range(2):
            for side in range(2):
                real = weights[level, side, half, 0]
                imag = weights[level, side, half, 1]
                i = half * 2 * ANGLES
                j = side * 2 * ANGLES
                big[level, i : i + ANGLES, j : j + ANGLES] = real
                big[level, i : i + ANGLES, j + ANGLES : j + 2 * ANGLES] = -imag
                big[level, i + ANGLES : i + 2 * ANGLES, j : j + ANGLES] = imag
                big[level, i + ANGLES : i + 2 * ANGLES, j + ANGLES : j + 2 * ANGLES] = real
            if level < LEVELS - 1:
                for part in range(2):
                    for start in range(0, rows, PERIOD):
                        size = min(PERIOD, rows - start)
                        table[level, half, part, start : start + size, :] = rows_table[
                            level, half, part, :size, :
                        ]

    eye = unit(LANES, 0)

    @pl.when(twin == origin)
    def _():
        raw[me] = image[:, mine, :, lanes(twin * block, tiles)]

    def await_part(part, count):
        for src in range(n):

            @pl.when(differs(src, first + origin))
            def _():
                part_arrival(src, part, count).wait_recv()

    def take(j):
        start = tile_of(twin, j) * LANES
        for src in range(n):
            for c in range(2):
                xt[src, c, pl.ds(pl.multiple_of(HALO + start, HALO), LANES), :] = lax.dot_general(
                    eye, raw[src, c, :, lanes(start)], NT, preferred_element_type=jnp.float32
                )

    await_part(0, 2)
    take(0)

    await_signal(met, meets_right)
    halo_at = pl.ds(pl.multiple_of(twin * (block + HALO), HALO), HALO)

    @pl.when(meets)
    def _():
        meet_copy().start()
        meet_copy().wait()

    @pl.when(inner)
    def _():
        for src in range(n):

            @pl.when(src != me)
            def _():
                edge_copy(0, src).wait_recv()

        xt[:, :, halo_at, :] = halo[...].astype(jnp.float32)

    @pl.when(jnp.logical_or(at_left, at_right))
    def _():
        xt[:, :, halo_at, :] = jnp.zeros((n, 2, HALO, ANGLES), jnp.float32)

    def send_back(j, s):
        here = jnp.logical_and(s == me, origin == twin)

        last = s % half_size > 0

        @pl.when(jnp.logical_and(jnp.logical_not(here), jnp.logical_or(j < tiles - 2, jnp.logical_not(last))))
        def _():
            out_copy(j, 1, s).start()

        @pl.when(jnp.logical_and(jnp.logical_not(here), jnp.logical_and(j == tiles - 1, last)))
        def _():
            out_copy(tiles - 2, 2, s).start()

        @pl.when(here)
        def _():
            cols = tile_of(twin, j) * LANES
            out[:, mine, :, lanes(twin * block + cols)] = stage[s, :, :, lanes(cols)]

    def per_tile(j, carry):
        @pl.when(jnp.logical_and(j > 0, j < tiles - 1))
        def _():
            await_part(j, 1)

        @pl.when(j < tiles - 1)
        def _():
            take(j + 1)

        @pl.when(j == tiles - 2)
        def _():
            twin_copy().start()

        @pl.when(j == tiles - 1)
        def _():
            twin_copy().wait()

        start = pl.multiple_of(tile_of(twin, j) * LANES, LANES)

        for level in range(LEVELS):
            mask = 2 ** (level % bits)
            base = RIM * level
            count = rows - 2 * base
            kept = count - 2 * RIM
            wide = kept + RIM

            pairs = [(p // mask * (2 * mask) + p % mask) for p in range(n // 2)]
            for pair, low in enumerate(pairs):
                members = (low, low + mask)
                for side in range(2):
                    k = shifts[level, side][None, :] + RIM
                    on8, on4, on2, on1 = [(k // p) % 2 == 1 for p in (8, 4, 2, 1)]
                    for c in range(2):
                        s = members[side]
                        b = side * 2 + c
                        held = xf.at[s, c] if level else xt.at[s, c, pl.ds(start, rows + 8)]
                        u = None
                        for t in range(TAPS):
                            term = taps[level, t] * held[pl.ds(base + t, count), :]
                            u = term if u is None else u + term
                        v = jnp.where(on8, u[RIM:], u[:wide])
                        sh0[b, :wide] = v
                        v = jnp.where(on4, sh0[b, pl.ds(4, wide), :], v)
                        sh1[b, :wide] = v
                        v = jnp.where(on2, sh1[b, pl.ds(2, wide), :], v)
                        sh2[b, :wide] = v
                        v = jnp.where(on1, sh2[b, pl.ds(1, kept), :], v[:kept])
                        i = b * ANGLES
                        ybuf[pair * kept : (pair + 1) * kept, i : i + ANGLES] = v.astype(jnp.bfloat16)
            y = ybuf[: n // 2 * kept, :]
            if level < LEVELS - 1:
                z = lax.dot_general(y, big[level], NT, preferred_element_type=jnp.float32)
                for pair, low in enumerate(pairs):
                    for half in range(2):
                        s = low + half * mask
                        i = half * 2 * ANGLES
                        r = pair * kept
                        re = z[r : r + kept, i : i + ANGLES]
                        im = z[r : r + kept, i + ANGLES : i + 2 * ANGLES]
                        span_rows = pl.ds(base + RIM, kept)
                        cosine = table[level, half, 0, span_rows, :]
                        sinus = table[level, half, 1, span_rows, :]
                        xf[s, 0, span_rows, :] = re * cosine - im * sinus
                        xf[s, 1, span_rows, :] = re * sinus + im * cosine
            else:
                z = lax.dot_general(big[level], y, NT, preferred_element_type=jnp.float32)
                for pair, low in enumerate(pairs):
                    for half in range(2):
                        s = low + half * mask
                        i = half * 2 * ANGLES
                        cosine, sinus = cols_table[half, 0], cols_table[half, 1]
                        r = pair * kept
                        re = z[i : i + ANGLES, r : r + kept]
                        im = z[i + ANGLES : i + 2 * ANGLES, r : r + kept]
                        stage[s, 0, :, lanes(start)] = (re * cosine - im * sinus).astype(jnp.bfloat16)
                        stage[s, 1, :, lanes(start)] = (re * sinus + im * cosine).astype(jnp.bfloat16)
                for low in pairs:
                    send_back(j, low + mask * (1 - mine))
                for low in pairs:
                    send_back(j, low + mask * mine)

            if level < LEVELS - 1:

                @pl.when(jnp.logical_and(at_left, j == 0))
                def _():
                    xf[:, :, :HALO, :] = jnp.zeros((n, 2, HALO, ANGLES), jnp.float32)

                @pl.when(jnp.logical_and(at_right, j == 0))
                def _():
                    xf[:, :, rows - HALO : rows, :] = jnp.zeros((n, 2, HALO, ANGLES), jnp.float32)

        return carry

    lax.fori_loop(0, tiles, per_tile, 0)

    for part in range(tiles - 1):
        for core in range(CORES):
            part_copy(1 - mine, core, part).wait_send()

            @pl.when(differs(mine * half_size + home, first + core))
            def _():
                part_copy(mine, core, part).wait_send()

    for m in range(2):

        @pl.when(m * half_size + 1 - home != me)
        def _():
            edge_copy(m, me).wait_send()

    merges = spot > 0
    for j in range(tiles):
        for z in range(n):
            if j < tiles - 2 or z % half_size == 0:

                @pl.when(differs(z, first + origin))
                def _():
                    out_copy(j, 1, z).wait_send()

            elif j == tiles - 2:

                @pl.when(differs(z, first + origin))
                def _():
                    out_copy(j, 2, z).wait_send()

        for h in range(2):
            for core in range(CORES):
                arrives = differs(h * half_size + home, first + core)
                if j < tiles - 2:

                    @pl.when(arrives)
                    def _():
                        out_arrival(h, core, j, 1).wait_recv()

                else:

                    @pl.when(jnp.logical_and(arrives, jnp.logical_not(merges)))
                    def _():
                        out_arrival(h, core, j, 1).wait_recv()

                    if j == tiles - 2:

                        @pl.when(jnp.logical_and(arrives, merges))
                        def _():
                            out_arrival(h, core, j, 2).wait_recv()


def in_one_kernel(n, rngs, image, interp_weights, range_taps, range_shifts):
    width = image.shape[3]
    block = 2 * width // n
    tiles = block // LANES
    rows = LANES + 2 * HALO
    rows_table, cols_table = phase_tables()
    vmem = pl.BlockSpec(memory_space=pltpu.VMEM)
    hbm = pl.BlockSpec(memory_space=pl.ANY)
    dma = pltpu.SemaphoreType.DMA
    f32, bf16 = jnp.float32, jnp.bfloat16
    return pl.pallas_call(
        functools.partial(merge_kernel, n, rngs),
        out_shape=pltpu.VMEM(image.shape, bf16),
        in_specs=[hbm] * 6,
        out_specs=vmem,
        scratch_shapes=[
            pltpu.VMEM(image.shape, bf16),
            pltpu.VMEM(interp_weights.shape, bf16),
            pltpu.SMEM(range_taps.shape, f32),
            pltpu.VMEM(range_shifts.shape, jnp.int32),
            pltpu.VMEM(rows_table.shape, f32),
            pltpu.VMEM(cols_table.shape, f32),
            dma((9,)),
            pltpu.VMEM((n, 2, ANGLES, block), bf16),
            pltpu.VMEM((n, 2, block + 2 * HALO + 8, ANGLES), f32),
            pltpu.VMEM((2, 2, HALO, ANGLES), bf16),
            pltpu.VMEM((n, 2, HALO, ANGLES), bf16),
            pltpu.VMEM((LEVELS, 4 * ANGLES, 4 * ANGLES), bf16),
            pltpu.VMEM((LEVELS - 1, 2, 2, rows, ANGLES), f32),
            pltpu.VMEM((n, 2, rows + 8, ANGLES), f32),
            pltpu.VMEM((4, rows + 8, ANGLES), f32),
            pltpu.VMEM((4, rows + 8, ANGLES), f32),
            pltpu.VMEM((4, rows + 8, ANGLES), f32),
            pltpu.VMEM((n // 2 * rows, 4 * ANGLES), bf16),
            pltpu.VMEM((n, 2, ANGLES, block), bf16),
            dma((2, CORES, tiles - 1)),
            dma((n, tiles - 1)),
            dma((2,)),
            dma((n,)),
            dma(()),
            dma(()),
            dma((tiles, n)),
            dma((2, CORES, tiles)),
            dma(()),
            dma(()),
            pltpu.SemaphoreType.REGULAR((n,)),
            pltpu.SemaphoreType.REGULAR,
        ],
        compiler_params=pltpu.CompilerParams(has_side_effects=True, collective_id=0),
    )(image, interp_weights, range_taps, range_shifts, rows_table, cols_table)


def fits_kernel(mesh, image_shape):
    n = mesh.shape["sub"]
    paired = mesh.shape["rng"] % CORES == 0
    tiled = image_shape[3] % (CORES * LANES) == 0 and image_shape[3] > CORES * LANES
    return paired and n == 2 * CORES and image_shape[1] == 2 and tiled and ANGLES == LANES


def per_device(mesh, image, *rest):
    if fits_kernel(mesh, image.shape):
        return in_one_kernel(mesh.shape["sub"], mesh.shape["rng"], image, *rest)
    return on_device(image, *rest)


def solution(mesh):
    return jax.shard_map(
        functools.partial(per_device, mesh),
        mesh=mesh,
        in_specs=(P(None, ("img", "sub"), None, "rng"), P(), P(), P()),
        out_specs=P(None, ("img", "sub"), None, "rng"),
        check_vma=False,
    )
```

```python
import math

import functools

import jax
import jax.numpy as jnp
import numpy as np
from jax import lax
from jax.experimental import pallas as pl
from jax.experimental.pallas import tpu as pltpu
from jax.sharding import PartitionSpec as P

ANGLES = 128
RANGE = 4096
RIM = 8
TAPS = 4
LEVELS = 4


phase_step = 2.0 * math.pi / 64.0


def padded_2(cells, sides, width):
    for axis, dim in sides:
        count = lax.axis_size(axis)
        ends = count - 1
        head = lax.slice_in_dim(cells, 0, width, axis=dim)
        tail = lax.slice_in_dim(cells, cells.shape[dim] - width, cells.shape[dim], axis=dim)
        cells = jnp.concatenate(
            [
                lax.ppermute(tail, axis, [(i, (i + 1) % count) for i in range(ends)]),
                cells,
                lax.ppermute(head, axis, [((i + 1) % count, i) for i in range(ends)]),
            ],
            axis=dim,
        )
    return cells


def from_partner(value, axis, stride):
    mask = 2**stride
    pairs = [(source, source ^ mask) for source in range(lax.axis_size(axis))]
    return lax.ppermute(value, axis, pairs)


def rotate(merged_sum, level_index, half_index, range_start, range_width):
    angle_rows = half_index * ANGLES + jnp.arange(ANGLES, dtype=jnp.int32)
    range_cols = range_start + jnp.arange(range_width, dtype=jnp.int32)
    wrapped = range_cols[None, :] * (angle_rows[:, None] + 1) * (7 + level_index) % 64
    phase = wrapped.astype(jnp.float32) * phase_step
    cosine = jnp.cos(phase)
    sinus = jnp.sin(phase)
    return jnp.stack(
        [
            merged_sum[0] * cosine - merged_sum[1] * sinus,
            merged_sum[0] * sinus + merged_sum[1] * cosine,
        ]
    )


def level_coef(range_taps, range_shifts, level_index, side_index):
    offsets = jnp.arange(2 * RIM + 1, dtype=jnp.int32) - RIM
    tap_ids = jnp.arange(TAPS, dtype=jnp.int32)
    hits = (
        range_shifts[level_index, side_index][:, None, None] + tap_ids[None, :, None]
        == offsets[None, None, :]
    )
    return jnp.einsum(
        "t,ato->ao",
        range_taps[level_index],
        hits.astype(jnp.float32),
        precision=lax.Precision.HIGHEST,
    )


def interpolate(padded, coef, range_width):
    total = None
    for offset_index in range(2 * RIM + 1):
        term = coef[:, offset_index, None] * padded[
            ..., offset_index : offset_index + range_width
        ].astype(jnp.float32)
        total = term if total is None else total + term
    return total.astype(jnp.bfloat16)


def block_of(weight_pair):
    return jnp.stack(
        [jnp.stack([weight_pair[0], -weight_pair[1]]), jnp.stack([weight_pair[1], weight_pair[0]])]
    )


def combine_sides(lower_rows, upper_rows, weights_level, half_index):
    chosen = lax.dynamic_index_in_dim(weights_level, half_index, 1, keepdims=False)
    merged_sum = None
    for side_index, source in ((0, lower_rows), (1, upper_rows)):
        product = jnp.einsum(
            "xcij,cgjr->xgir",
            block_of(chosen[side_index]),
            source,
            preferred_element_type=jnp.float32,
        )
        merged_sum = product if merged_sum is None else merged_sum + product
    return merged_sum


def on_device(image, interp_weights, range_taps, range_shifts):
    range_width = image.shape[3]
    sub_count = lax.axis_size("sub")
    bit_count = sub_count.bit_length() - 1
    sub_index = lax.axis_index("sub")
    range_start = lax.axis_index("rng") * range_width
    current = padded_2(image, (("rng", 3),), LEVELS * RIM)
    margin = LEVELS * RIM
    for level_index in range(LEVELS):
        bit = level_index % bit_count
        own_half = sub_index // 2**bit % 2
        padded = current
        margin = margin - RIM
        out_width = range_width + 2 * margin
        coef = jnp.where(
            own_half == 0,
            level_coef(range_taps, range_shifts, level_index, 0),
            level_coef(range_taps, range_shifts, level_index, 1),
        )
        own_rows = interpolate(padded, coef, out_width)
        partner = from_partner(own_rows, "sub", bit)
        lower_rows = jnp.where(own_half == 0, own_rows, partner)
        upper_rows = jnp.where(own_half == 0, partner, own_rows)
        merged = combine_sides(lower_rows, upper_rows, interp_weights[level_index], own_half)
        turned = rotate(merged, level_index, own_half, range_start - margin, out_width)
        global_cols = range_start - margin + jnp.arange(out_width, dtype=jnp.int32)
        inside = jnp.logical_and(global_cols >= 0, global_cols < RANGE)
        turned = jnp.where(inside, turned, 0.0)
        current = turned.astype(jnp.bfloat16)
    return current


PERIOD = 64
LANES = 128
CORES = 2
HALO = LEVELS * RIM
MESH = pl.DeviceIdType.MESH
NT = (((1,), (1,)), ((), ()))


def phase_tables():
    a = np.arange(ANGLES)
    tables = np.zeros((LEVELS, 2, 2, PERIOD, ANGLES), np.float32)
    for level in range(LEVELS):
        for half in range(2):
            start = -HALO if level < LEVELS - 1 else 0
            r = (start + np.arange(PERIOD))[:, None]
            wrapped = (r * (half * ANGLES + a + 1)[None, :] * (7 + level)) % PERIOD
            phase = wrapped * phase_step
            tables[level, half, 0] = np.cos(phase)
            tables[level, half, 1] = np.sin(phase)
    last = np.swapaxes(tables[LEVELS - 1], -1, -2)
    last = np.concatenate([last] * (LANES // PERIOD), -1)
    return tables[: LEVELS - 1], last


def tile_parts(tiles):
    return [(0, 2), *[(j, 1) for j in range(2, tiles)]]


def merge_kernel(
    n, rngs, image_hbm, weights_hbm, taps_hbm, shifts_hbm, rows_hbm, cols_hbm, out,
    image, weights, taps, shifts, rows_table, cols_table, load_sem,
    raw, xt, big, table, xf, sh0, sh1, sh2, ybuf, stage,
    tile_send, tile_recv, twin_send, twin_recv, out_send, out_recv,
    rim_send, rim_recv, seen, met,
):
    me = lax.axis_index("sub")
    place = lax.axis_index("rng")
    width = image_hbm.shape[3]
    half_size = n // 2
    block = 2 * width // n
    tiles = block // LANES
    rows = LANES + 2 * HALO
    bits = n.bit_length() - 1
    pairs = [(j, min(2, tiles - j)) for j in range(0, tiles, 2)]
    parts = tile_parts(tiles)
    plans = ([(j, 1) for j in range(tiles)], [*[(j, 1) for j in range(pairs[-1][0])], pairs[-1]])

    twin = place % CORES
    first = place - twin
    mine = me // half_size
    spot = me % half_size
    flip = place // CORES % 2
    home = twin + flip * (1 - 2 * twin)
    origin = spot + flip * (1 - 2 * spot)
    inner = twin != origin
    at_left = jnp.logical_and(place == 0, origin == 0)
    at_right = jnp.logical_and(place == rngs - 1, origin == CORES - 1)
    meets = jnp.logical_not(jnp.logical_or(inner, jnp.logical_or(at_left, at_right)))
    meets_right = jnp.logical_and(meets, twin == 1)
    meets_left = jnp.logical_and(meets, twin == 0)
    across = 1 - 2 * twin
    rim_sub = jnp.where(inner, mine * half_size + half_size - 1 - spot, me)
    rim_rng = jnp.where(inner, place + across, place - across)

    def tile_of(core, j):
        return j + core * (tiles - 1 - 2 * j)

    def lanes(start, count=1):
        return pl.ds(pl.multiple_of(start, LANES), count * LANES)

    def columns(core, j, count=1):
        return tile_of(core, j) * LANES - core * (count - 1) * LANES

    def part_copy(m, core, part, source=None):
        j, count = parts[part]
        start = columns(core, j, count)
        return pltpu.make_async_remote_copy(
            src_ref=(image if source is None else source).at[:, m, :, lanes(core * block + start, count)],
            dst_ref=raw.at[me, :, :, lanes(start, count)],
            send_sem=tile_send.at[m, core, part],
            recv_sem=tile_recv.at[me, part],
            device_id={"sub": m * half_size + home, "rng": first + core},
            device_id_type=MESH,
        )

    def part_arrival(src, part, count):
        here = raw.at[src, :, :, lanes(0, count)]
        return pltpu.make_async_remote_copy(
            src_ref=here,
            dst_ref=here,
            send_sem=tile_send.at[0, 0, 0],
            recv_sem=tile_recv.at[src, part],
            device_id={"sub": src, "rng": first + origin},
            device_id_type=MESH,
        )

    def rim_copy():
        return pltpu.make_async_remote_copy(
            src_ref=xt.at[:, :, pl.ds(pl.multiple_of(HALO + twin * (block - HALO), HALO), HALO), :],
            dst_ref=xt.at[
                :, :, pl.ds(pl.multiple_of((1 - twin) * (block + HALO), HALO), HALO), :
            ],
            send_sem=rim_send,
            recv_sem=rim_recv,
            device_id={"sub": rim_sub, "rng": rim_rng},
            device_id_type=MESH,
        )

    def twin_copy():
        return pltpu.make_async_remote_copy(
            src_ref=xt.at[:, :, pl.ds(pl.multiple_of(block - twin * (block - HALO), HALO), HALO), :],
            dst_ref=xt.at[:, :, pl.ds(pl.multiple_of(twin * (block + HALO), HALO), HALO), :],
            send_sem=twin_send,
            recv_sem=twin_recv,
            device_id={"rng": place + 1 - 2 * twin},
            device_id_type=MESH,
        )

    def out_copy(j, count, z):
        start = columns(twin, j, count)
        return pltpu.make_async_remote_copy(
            src_ref=stage.at[z, :, :, lanes(start, count)],
            dst_ref=out.at[:, mine, :, lanes(twin * block + start, count)],
            send_sem=out_send.at[j, z],
            recv_sem=out_recv.at[mine, twin, j],
            device_id={"sub": z, "rng": first + origin},
            device_id_type=MESH,
        )

    def out_arrival(h, core, j, count):
        here = out.at[:, h, :, lanes(core * block + columns(core, j, count), count)]
        return pltpu.make_async_remote_copy(
            src_ref=here,
            dst_ref=here,
            send_sem=out_send.at[0, 0],
            recv_sem=out_recv.at[h, core, j],
            device_id={"sub": h * half_size + home, "rng": first + core},
            device_id_type=MESH,
        )

    def differs(z, r):
        return jnp.logical_or(me != z, place != r)

    def signal(sem, cond, z, r):
        @pl.when(cond)
        def _():
            pl.semaphore_signal(sem, inc=1, device_id={"sub": z, "rng": r}, device_id_type=MESH)

    def await_signal(sem, cond, count=1):
        @pl.when(cond)
        def _():
            pl.semaphore_wait(sem, count)

    def load(k, m, start, size):
        cols = pl.ds(start, size)
        return pltpu.make_async_copy(image_hbm.at[:, m, :, cols], image.at[:, m, :, cols], load_sem.at[k])

    loads = [
        load(0, 1 - mine, 0, 2 * LANES),
        load(1, 1 - mine, width - 2 * LANES, 2 * LANES),
        load(2, mine, 0, width),
    ]
    if width > 4 * LANES:
        loads.append(load(3, 1 - mine, 2 * LANES, width - 4 * LANES))
    others = [
        pltpu.make_async_copy(src, dst, load_sem.at[4 + k])
        for k, (src, dst) in enumerate(
            (
                (weights_hbm, weights),
                (rows_hbm, rows_table),
                (cols_hbm, cols_table),
                (taps_hbm, taps),
                (shifts_hbm, shifts),
            )
        )
    ]
    for copy in loads + others:
        copy.start()

    barrier = pltpu.get_barrier_semaphore()
    for step in range(1, n):
        for c in range(CORES):
            signal(barrier, me + step < n, me + step, first + c)
    pl.semaphore_signal(
        barrier, inc=1, device_id={"rng": place + across}, device_id_type=MESH
    )
    signal(barrier, meets_right, me, place + 1)

    def send_across(part):
        for core in range(CORES):
            part_copy(1 - mine, core, part).start()

    def send_along(part):
        for core in range(CORES):

            @pl.when(differs(mine * half_size + home, first + core))
            def _():
                part_copy(mine, core, part).start()

    pl.semaphore_wait(barrier, 1 + CORES * me + meets_left.astype(jnp.int32))
    for step in range(1, n):
        for c in range(CORES):
            signal(seen.at[step], me - step >= 0, me - step, first + c)
    signal(met, meets_left, me, place - 1)

    @pl.when(mine == 1)
    def _():
        for core in range(CORES):
            part_copy(1 - mine, core, 0, image_hbm).start()

    loads[0].wait()
    loads[1].wait()

    loads[2].wait()

    @pl.when(home <= spot)
    def _():
        send_along(0)

    for copy in loads[3:]:
        copy.wait()
    for step in range(1, n):
        await_signal(seen.at[step], me + step < n, CORES)

        @pl.when(jnp.logical_and(mine == 0, half_size + home - me == step))
        def _():
            send_across(0)

        if step == 1:

            @pl.when(home > spot)
            def _():
                send_along(0)

    def unit(count, shift):
        i = lax.broadcasted_iota(jnp.int32, (count, LANES), 0)
        k = lax.broadcasted_iota(jnp.int32, (count, LANES), 1)
        return (i + shift == k).astype(jnp.bfloat16)

    for part in range(1, len(parts) - 1):
        send_across(part)
        send_along(part)

    for copy in others:
        copy.wait()

    for level in range(LEVELS):
        for half in range(2):
            for side in range(2):
                real = weights[level, side, half, 0]
                imag = weights[level, side, half, 1]
                i = half * 2 * ANGLES
                j = side * 2 * ANGLES
                big[level, i : i + ANGLES, j : j + ANGLES] = real
                big[level, i : i + ANGLES, j + ANGLES : j + 2 * ANGLES] = -imag
                big[level, i + ANGLES : i + 2 * ANGLES, j : j + ANGLES] = imag
                big[level, i + ANGLES : i + 2 * ANGLES, j + ANGLES : j + 2 * ANGLES] = real
            if level < LEVELS - 1:
                for part in range(2):
                    for start in range(0, rows, PERIOD):
                        size = min(PERIOD, rows - start)
                        table[level, half, part, start : start + size, :] = rows_table[
                            level, half, part, :size, :
                        ]

    eye = unit(LANES, 0)

    @pl.when(twin == origin)
    def _():
        raw[me] = image[:, mine, :, lanes(twin * block, tiles)]

    def await_part(part, count):
        for src in range(n):

            @pl.when(differs(src, first + origin))
            def _():
                part_arrival(src, part, count).wait_recv()

    def take(j):
        start = tile_of(twin, j) * LANES
        for src in range(n):
            for c in range(2):
                xt[src, c, pl.ds(pl.multiple_of(HALO + start, HALO), LANES), :] = lax.dot_general(
                    eye, raw[src, c, :, lanes(start)], NT, preferred_element_type=jnp.float32
                )

    await_part(0, parts[0][1])
    take(0)

    await_signal(met, meets_right)
    halo_at = pl.ds(pl.multiple_of(twin * (block + HALO), HALO), HALO)
    ends = jnp.logical_or(at_left, at_right)

    @pl.when(jnp.logical_not(ends))
    def _():
        rim_copy().start()

    for part in range(max(1, len(parts) - 1), len(parts)):
        send_across(part)
        send_along(part)

    @pl.when(jnp.logical_not(ends))
    def _():
        rim_copy().wait()

    @pl.when(ends)
    def _():
        xt[:, :, halo_at, :] = jnp.zeros((n, 2, HALO, ANGLES), jnp.float32)

    def send_back(j, s, far):
        here = jnp.logical_and(s == me, origin == twin)
        for start, count in plans[far]:

            @pl.when(jnp.logical_and(jnp.logical_not(here), j == start + count - 1))
            def _():
                out_copy(start, count, s).start()

        @pl.when(here)
        def _():
            cols = tile_of(twin, j) * LANES
            out[:, mine, :, lanes(twin * block + cols)] = stage[s, :, :, lanes(cols)]

    def per_tile(j, carry):
        for part in range(1, len(parts)):

            @pl.when(j + 1 == parts[part][0])
            def _():
                await_part(part, parts[part][1])

        @pl.when(j < tiles - 1)
        def _():
            take(j + 1)

        @pl.when(j == tiles - 2)
        def _():
            twin_copy().start()

        @pl.when(j == tiles - 1)
        def _():
            twin_copy().wait()

        start = pl.multiple_of(tile_of(twin, j) * LANES, LANES)

        for level in range(LEVELS):
            mask = 2 ** (level % bits)
            base = RIM * level
            count = rows - 2 * base
            kept = count - 2 * RIM
            wide = kept + RIM

            pairs = [(p // mask * (2 * mask) + p % mask) for p in range(n // 2)]
            for pair, low in enumerate(pairs):
                members = (low, low + mask)
                for side in range(2):
                    k = shifts[level, side][None, :] + RIM
                    on8, on4, on2, on1 = [(k // p) % 2 == 1 for p in (8, 4, 2, 1)]
                    for c in range(2):
                        s = members[side]
                        b = side * 2 + c
                        held = xf.at[s, c] if level else xt.at[s, c, pl.ds(start, rows + 8)]
                        u = None
                        for t in range(TAPS):
                            term = taps[level, t] * held[pl.ds(base + t, count), :]
                            u = term if u is None else u + term
                        v = jnp.where(on8, u[RIM:], u[:wide])
                        sh0[b, :wide] = v
                        v = jnp.where(on4, sh0[b, pl.ds(4, wide), :], v)
                        sh1[b, :wide] = v
                        v = jnp.where(on2, sh1[b, pl.ds(2, wide), :], v)
                        sh2[b, :wide] = v
                        v = jnp.where(on1, sh2[b, pl.ds(1, kept), :], v[:kept])
                        i = b * ANGLES
                        ybuf[pair * kept : (pair + 1) * kept, i : i + ANGLES] = v.astype(jnp.bfloat16)
            y = ybuf[: n // 2 * kept, :]
            if level < LEVELS - 1:
                z = lax.dot_general(y, big[level], NT, preferred_element_type=jnp.float32)
                for pair, low in enumerate(pairs):
                    for half in range(2):
                        s = low + half * mask
                        i = half * 2 * ANGLES
                        r = pair * kept
                        re = z[r : r + kept, i : i + ANGLES]
                        im = z[r : r + kept, i + ANGLES : i + 2 * ANGLES]
                        span_rows = pl.ds(base + RIM, kept)
                        cosine = table[level, half, 0, span_rows, :]
                        sinus = table[level, half, 1, span_rows, :]
                        xf[s, 0, span_rows, :] = re * cosine - im * sinus
                        xf[s, 1, span_rows, :] = re * sinus + im * cosine
            else:
                z = lax.dot_general(big[level], y, NT, preferred_element_type=jnp.float32)
                for pair, low in enumerate(pairs):
                    for half in range(2):
                        s = low + half * mask
                        i = half * 2 * ANGLES
                        cosine, sinus = cols_table[half, 0], cols_table[half, 1]
                        r = pair * kept
                        re = z[i : i + ANGLES, r : r + kept]
                        im = z[i + ANGLES : i + 2 * ANGLES, r : r + kept]
                        stage[s, 0, :, lanes(start)] = (re * cosine - im * sinus).astype(jnp.bfloat16)
                        stage[s, 1, :, lanes(start)] = (re * sinus + im * cosine).astype(jnp.bfloat16)
                for group in (1 - mine, mine):
                    for spot_to in range(half_size):
                        send_back(j, group * half_size + spot_to, spot_to > 0)

            if level < LEVELS - 1:

                @pl.when(jnp.logical_and(at_left, j == 0))
                def _():
                    xf[:, :, :HALO, :] = jnp.zeros((n, 2, HALO, ANGLES), jnp.float32)

                @pl.when(jnp.logical_and(at_right, j == 0))
                def _():
                    xf[:, :, rows - HALO : rows, :] = jnp.zeros((n, 2, HALO, ANGLES), jnp.float32)

        return carry

    lax.fori_loop(0, tiles, per_tile, 0)

    for part in range(len(parts)):
        for core in range(CORES):
            part_copy(1 - mine, core, part).wait_send()

            @pl.when(differs(mine * half_size + home, first + core))
            def _():
                part_copy(mine, core, part).wait_send()

    for far, plan in enumerate(plans):
        for start, count in plan:
            for z in range(n):
                if (z % half_size > 0) == far:

                    @pl.when(differs(z, first + origin))
                    def _():
                        out_copy(start, count, z).wait_send()

            for h in range(2):
                for core in range(CORES):
                    arrives = differs(h * half_size + home, first + core)

                    @pl.when(jnp.logical_and(arrives, (spot > 0) == far))
                    def _():
                        out_arrival(h, core, start, count).wait_recv()


def in_one_kernel(n, rngs, image, interp_weights, range_taps, range_shifts):
    width = image.shape[3]
    block = 2 * width // n
    tiles = block // LANES
    rows = LANES + 2 * HALO
    parts = len(tile_parts(tiles))
    rows_table, cols_table = phase_tables()
    vmem = pl.BlockSpec(memory_space=pltpu.VMEM)
    hbm = pl.BlockSpec(memory_space=pl.ANY)
    dma = pltpu.SemaphoreType.DMA
    f32, bf16 = jnp.float32, jnp.bfloat16
    return pl.pallas_call(
        functools.partial(merge_kernel, n, rngs),
        out_shape=pltpu.VMEM(image.shape, bf16),
        in_specs=[hbm] * 6,
        out_specs=vmem,
        scratch_shapes=[
            pltpu.VMEM(image.shape, bf16),
            pltpu.VMEM(interp_weights.shape, bf16),
            pltpu.SMEM(range_taps.shape, f32),
            pltpu.VMEM(range_shifts.shape, jnp.int32),
            pltpu.VMEM(rows_table.shape, f32),
            pltpu.VMEM(cols_table.shape, f32),
            dma((9,)),
            pltpu.VMEM((n, 2, ANGLES, block), bf16),
            pltpu.VMEM((n, 2, block + 2 * HALO + 8, ANGLES), f32),
            pltpu.VMEM((LEVELS, 4 * ANGLES, 4 * ANGLES), bf16),
            pltpu.VMEM((LEVELS - 1, 2, 2, rows, ANGLES), f32),
            pltpu.VMEM((n, 2, rows + 8, ANGLES), f32),
            pltpu.VMEM((4, rows + 8, ANGLES), f32),
            pltpu.VMEM((4, rows + 8, ANGLES), f32),
            pltpu.VMEM((4, rows + 8, ANGLES), f32),
            pltpu.VMEM((n // 2 * rows, 4 * ANGLES), bf16),
            pltpu.VMEM((n, 2, ANGLES, block), bf16),
            dma((2, CORES, parts)),
            dma((n, parts)),
            dma(()),
            dma(()),
            dma((tiles, n)),
            dma((2, CORES, tiles)),
            dma(()),
            dma(()),
            pltpu.SemaphoreType.REGULAR((n,)),
            pltpu.SemaphoreType.REGULAR,
        ],
        compiler_params=pltpu.CompilerParams(has_side_effects=True, collective_id=0),
    )(image, interp_weights, range_taps, range_shifts, rows_table, cols_table)


def fits_kernel(mesh, image_shape):
    n = mesh.shape["sub"]
    paired = mesh.shape["rng"] % CORES == 0
    tiled = image_shape[3] % (CORES * LANES) == 0 and image_shape[3] > CORES * LANES
    return paired and n == 2 * CORES and image_shape[1] == 2 and tiled and ANGLES == LANES


def per_device(mesh, image, *rest):
    if fits_kernel(mesh, image.shape):
        return in_one_kernel(mesh.shape["sub"], mesh.shape["rng"], image, *rest)
    return on_device(image, *rest)


def solution(mesh):
    return jax.shard_map(
        functools.partial(per_device, mesh),
        mesh=mesh,
        in_specs=(P(None, ("img", "sub"), None, "rng"), P(), P(), P()),
        out_specs=P(None, ("img", "sub"), None, "rng"),
        check_vma=False,
    )
```

```python
import math

import functools

import jax
import jax.numpy as jnp
import numpy as np
from jax import lax
from jax.experimental import pallas as pl
from jax.experimental.pallas import tpu as pltpu
from jax.sharding import PartitionSpec as P

ANGLES = 128
RANGE = 4096
RIM = 8
TAPS = 4
LEVELS = 4


phase_step = 2.0 * math.pi / 64.0


def padded_2(cells, sides, width):
    for axis, dim in sides:
        count = lax.axis_size(axis)
        ends = count - 1
        head = lax.slice_in_dim(cells, 0, width, axis=dim)
        tail = lax.slice_in_dim(cells, cells.shape[dim] - width, cells.shape[dim], axis=dim)
        cells = jnp.concatenate(
            [
                lax.ppermute(tail, axis, [(i, (i + 1) % count) for i in range(ends)]),
                cells,
                lax.ppermute(head, axis, [((i + 1) % count, i) for i in range(ends)]),
            ],
            axis=dim,
        )
    return cells


def from_partner(value, axis, stride):
    mask = 2**stride
    pairs = [(source, source ^ mask) for source in range(lax.axis_size(axis))]
    return lax.ppermute(value, axis, pairs)


def rotate(merged_sum, level_index, half_index, range_start, range_width):
    angle_rows = half_index * ANGLES + jnp.arange(ANGLES, dtype=jnp.int32)
    range_cols = range_start + jnp.arange(range_width, dtype=jnp.int32)
    wrapped = range_cols[None, :] * (angle_rows[:, None] + 1) * (7 + level_index) % 64
    phase = wrapped.astype(jnp.float32) * phase_step
    cosine = jnp.cos(phase)
    sinus = jnp.sin(phase)
    return jnp.stack(
        [
            merged_sum[0] * cosine - merged_sum[1] * sinus,
            merged_sum[0] * sinus + merged_sum[1] * cosine,
        ]
    )


def level_coef(range_taps, range_shifts, level_index, side_index):
    offsets = jnp.arange(2 * RIM + 1, dtype=jnp.int32) - RIM
    tap_ids = jnp.arange(TAPS, dtype=jnp.int32)
    hits = (
        range_shifts[level_index, side_index][:, None, None] + tap_ids[None, :, None]
        == offsets[None, None, :]
    )
    return jnp.einsum(
        "t,ato->ao",
        range_taps[level_index],
        hits.astype(jnp.float32),
        precision=lax.Precision.HIGHEST,
    )


def interpolate(padded, coef, range_width):
    total = None
    for offset_index in range(2 * RIM + 1):
        term = coef[:, offset_index, None] * padded[
            ..., offset_index : offset_index + range_width
        ].astype(jnp.float32)
        total = term if total is None else total + term
    return total.astype(jnp.bfloat16)


def block_of(weight_pair):
    return jnp.stack(
        [jnp.stack([weight_pair[0], -weight_pair[1]]), jnp.stack([weight_pair[1], weight_pair[0]])]
    )


def combine_sides(lower_rows, upper_rows, weights_level, half_index):
    chosen = lax.dynamic_index_in_dim(weights_level, half_index, 1, keepdims=False)
    merged_sum = None
    for side_index, source in ((0, lower_rows), (1, upper_rows)):
        product = jnp.einsum(
            "xcij,cgjr->xgir",
            block_of(chosen[side_index]),
            source,
            preferred_element_type=jnp.float32,
        )
        merged_sum = product if merged_sum is None else merged_sum + product
    return merged_sum


def on_device(image, interp_weights, range_taps, range_shifts):
    range_width = image.shape[3]
    sub_count = lax.axis_size("sub")
    bit_count = sub_count.bit_length() - 1
    sub_index = lax.axis_index("sub")
    range_start = lax.axis_index("rng") * range_width
    current = padded_2(image, (("rng", 3),), LEVELS * RIM)
    margin = LEVELS * RIM
    for level_index in range(LEVELS):
        bit = level_index % bit_count
        own_half = sub_index // 2**bit % 2
        padded = current
        margin = margin - RIM
        out_width = range_width + 2 * margin
        coef = jnp.where(
            own_half == 0,
            level_coef(range_taps, range_shifts, level_index, 0),
            level_coef(range_taps, range_shifts, level_index, 1),
        )
        own_rows = interpolate(padded, coef, out_width)
        partner = from_partner(own_rows, "sub", bit)
        lower_rows = jnp.where(own_half == 0, own_rows, partner)
        upper_rows = jnp.where(own_half == 0, partner, own_rows)
        merged = combine_sides(lower_rows, upper_rows, interp_weights[level_index], own_half)
        turned = rotate(merged, level_index, own_half, range_start - margin, out_width)
        global_cols = range_start - margin + jnp.arange(out_width, dtype=jnp.int32)
        inside = jnp.logical_and(global_cols >= 0, global_cols < RANGE)
        turned = jnp.where(inside, turned, 0.0)
        current = turned.astype(jnp.bfloat16)
    return current


PERIOD = 64
LANES = 128
CORES = 2
HALO = LEVELS * RIM
MESH = pl.DeviceIdType.MESH
NT = (((1,), (1,)), ((), ()))


def phase_tables():
    a = np.arange(ANGLES)
    tables = np.zeros((LEVELS, 2, 2, PERIOD, ANGLES), np.float32)
    for level in range(LEVELS):
        for half in range(2):
            start = -HALO if level < LEVELS - 1 else 0
            r = (start + np.arange(PERIOD))[:, None]
            wrapped = (r * (half * ANGLES + a + 1)[None, :] * (7 + level)) % PERIOD
            phase = wrapped * phase_step
            tables[level, half, 0] = np.cos(phase)
            tables[level, half, 1] = np.sin(phase)
    last = np.swapaxes(tables[LEVELS - 1], -1, -2)
    last = np.concatenate([last] * (LANES // PERIOD), -1)
    return tables[: LEVELS - 1], last


def tile_parts(tiles):
    return [(0, 2), *[(j, 1) for j in range(2, tiles)]]


def merge_kernel(
    n, rngs, image_hbm, weights_hbm, taps_hbm, shifts_hbm, rows_hbm, cols_hbm, out,
    image, weights, taps, shifts, rows_table, cols_table, load_sem,
    raw, xt, big, table, xf, sh0, sh1, sh2, ybuf, stage,
    tile_send, tile_recv, twin_send, twin_recv, out_send, out_recv,
    rim_send, rim_recv, seen, met,
):
    me = lax.axis_index("sub")
    place = lax.axis_index("rng")
    width = image_hbm.shape[3]
    half_size = n // 2
    block = 2 * width // n
    tiles = block // LANES
    rows = LANES + 2 * HALO
    bits = n.bit_length() - 1
    pairs = [(j, min(2, tiles - j)) for j in range(0, tiles, 2)]
    parts = tile_parts(tiles)
    plans = ([(j, 1) for j in range(tiles)], [*[(j, 1) for j in range(pairs[-1][0])], pairs[-1]])

    twin = place % CORES
    first = place - twin
    mine = me // half_size
    spot = me % half_size
    flip = place // CORES % 2
    home = twin + flip * (1 - 2 * twin)
    origin = spot + flip * (1 - 2 * spot)
    inner = twin != origin
    at_left = jnp.logical_and(place == 0, origin == 0)
    at_right = jnp.logical_and(place == rngs - 1, origin == CORES - 1)
    meets = jnp.logical_not(jnp.logical_or(inner, jnp.logical_or(at_left, at_right)))
    meets_right = jnp.logical_and(meets, twin == 1)
    meets_left = jnp.logical_and(meets, twin == 0)
    across = 1 - 2 * twin
    rim_sub = jnp.where(inner, mine * half_size + half_size - 1 - spot, me)
    rim_rng = jnp.where(inner, place + across, place - across)

    def tile_of(core, j):
        return j + core * (tiles - 1 - 2 * j)

    def lanes(start, count=1):
        return pl.ds(pl.multiple_of(start, LANES), count * LANES)

    def columns(core, j, count=1):
        return tile_of(core, j) * LANES - core * (count - 1) * LANES

    def part_copy(m, core, part, source=None):
        j, count = parts[part]
        start = columns(core, j, count)
        return pltpu.make_async_remote_copy(
            src_ref=(image if source is None else source).at[:, m, :, lanes(core * block + start, count)],
            dst_ref=raw.at[me, :, :, lanes(start, count)],
            send_sem=tile_send.at[m, core, part],
            recv_sem=tile_recv.at[me, part],
            device_id={"sub": m * half_size + home, "rng": first + core},
            device_id_type=MESH,
        )

    def part_arrival(src, part, count):
        here = raw.at[src, :, :, lanes(0, count)]
        return pltpu.make_async_remote_copy(
            src_ref=here,
            dst_ref=here,
            send_sem=tile_send.at[0, 0, 0],
            recv_sem=tile_recv.at[src, part],
            device_id={"sub": src, "rng": first + origin},
            device_id_type=MESH,
        )

    def rim_copy():
        return pltpu.make_async_remote_copy(
            src_ref=xt.at[:, :, pl.ds(pl.multiple_of(HALO + twin * (block - HALO), HALO), HALO), :],
            dst_ref=xt.at[
                :, :, pl.ds(pl.multiple_of((1 - twin) * (block + HALO), HALO), HALO), :
            ],
            send_sem=rim_send,
            recv_sem=rim_recv,
            device_id={"sub": rim_sub, "rng": rim_rng},
            device_id_type=MESH,
        )

    def twin_copy():
        return pltpu.make_async_remote_copy(
            src_ref=xt.at[:, :, pl.ds(pl.multiple_of(block - twin * (block - HALO), HALO), HALO), :],
            dst_ref=xt.at[:, :, pl.ds(pl.multiple_of(twin * (block + HALO), HALO), HALO), :],
            send_sem=twin_send,
            recv_sem=twin_recv,
            device_id={"rng": place + 1 - 2 * twin},
            device_id_type=MESH,
        )

    def out_copy(j, count, z):
        start = columns(twin, j, count)
        return pltpu.make_async_remote_copy(
            src_ref=stage.at[z, :, :, lanes(start, count)],
            dst_ref=out.at[:, mine, :, lanes(twin * block + start, count)],
            send_sem=out_send.at[j, z],
            recv_sem=out_recv.at[mine, twin, j],
            device_id={"sub": z, "rng": first + origin},
            device_id_type=MESH,
        )

    def out_arrival(h, core, j, count):
        here = out.at[:, h, :, lanes(core * block + columns(core, j, count), count)]
        return pltpu.make_async_remote_copy(
            src_ref=here,
            dst_ref=here,
            send_sem=out_send.at[0, 0],
            recv_sem=out_recv.at[h, core, j],
            device_id={"sub": h * half_size + home, "rng": first + core},
            device_id_type=MESH,
        )

    def differs(z, r):
        return jnp.logical_or(me != z, place != r)

    def signal(sem, cond, z, r):
        @pl.when(cond)
        def _():
            pl.semaphore_signal(sem, inc=1, device_id={"sub": z, "rng": r}, device_id_type=MESH)

    def await_signal(sem, cond, count=1):
        @pl.when(cond)
        def _():
            pl.semaphore_wait(sem, count)

    def load(k, m, start, size):
        cols = pl.ds(start, size)
        return pltpu.make_async_copy(image_hbm.at[:, m, :, cols], image.at[:, m, :, cols], load_sem.at[k])

    loads = [
        load(0, 1 - mine, 0, 2 * LANES),
        load(1, 1 - mine, width - 2 * LANES, 2 * LANES),
        load(2, mine, 0, width),
    ]
    if width > 4 * LANES:
        loads.append(load(3, 1 - mine, 2 * LANES, width - 4 * LANES))
    others = [
        pltpu.make_async_copy(src, dst, load_sem.at[4 + k])
        for k, (src, dst) in enumerate(
            (
                (weights_hbm, weights),
                (rows_hbm, rows_table),
                (cols_hbm, cols_table),
                (taps_hbm, taps),
                (shifts_hbm, shifts),
            )
        )
    ]
    for copy in loads + others:
        copy.start()

    barrier = pltpu.get_barrier_semaphore()
    for step in range(1, n):
        for c in range(CORES):
            signal(barrier, me + step < n, me + step, first + c)
    pl.semaphore_signal(
        barrier, inc=1, device_id={"rng": place + across}, device_id_type=MESH
    )
    signal(barrier, meets_right, me, place + 1)

    def send_across(part):
        for core in range(CORES):
            part_copy(1 - mine, core, part).start()

    def send_along(part):
        for core in range(CORES):

            @pl.when(differs(mine * half_size + home, first + core))
            def _():
                part_copy(mine, core, part).start()

    pl.semaphore_wait(barrier, 1 + CORES * me + meets_left.astype(jnp.int32))
    for step in range(1, n):
        for c in range(CORES):
            signal(seen.at[step], me - step >= 0, me - step, first + c)
    signal(met, meets_left, me, place - 1)

    @pl.when(mine == 1)
    def _():
        for core in range(CORES):
            part_copy(1 - mine, core, 0, image_hbm).start()

    loads[0].wait()
    loads[1].wait()

    loads[2].wait()

    @pl.when(home <= spot)
    def _():
        send_along(0)

    for copy in loads[3:]:
        copy.wait()
    for step in range(1, n):
        await_signal(seen.at[step], me + step < n, CORES)

        @pl.when(jnp.logical_and(mine == 0, half_size + home - me == step))
        def _():
            send_across(0)

        if step == 1:

            @pl.when(home > spot)
            def _():
                send_along(0)

    def unit(count, shift):
        i = lax.broadcasted_iota(jnp.int32, (count, LANES), 0)
        k = lax.broadcasted_iota(jnp.int32, (count, LANES), 1)
        return (i + shift == k).astype(jnp.bfloat16)

    holds = me == half_size - 1

    def send_middle():
        for part in range(1, len(parts) - 1):
            send_across(part)
            send_along(part)

    @pl.when(jnp.logical_not(holds))
    def _():
        send_middle()

    for copy in others:
        copy.wait()

    for level in range(LEVELS):
        for half in range(2):
            for side in range(2):
                real = weights[level, side, half, 0]
                imag = weights[level, side, half, 1]
                i = half * 2 * ANGLES
                j = side * 2 * ANGLES
                big[level, i : i + ANGLES, j : j + ANGLES] = real
                big[level, i : i + ANGLES, j + ANGLES : j + 2 * ANGLES] = -imag
                big[level, i + ANGLES : i + 2 * ANGLES, j : j + ANGLES] = imag
                big[level, i + ANGLES : i + 2 * ANGLES, j + ANGLES : j + 2 * ANGLES] = real
            if level < LEVELS - 1:
                for part in range(2):
                    for start in range(0, rows, PERIOD):
                        size = min(PERIOD, rows - start)
                        table[level, half, part, start : start + size, :] = rows_table[
                            level, half, part, :size, :
                        ]

    eye = unit(LANES, 0)

    @pl.when(twin == origin)
    def _():
        raw[me] = image[:, mine, :, lanes(twin * block, tiles)]

    def await_part(part, count):
        for src in range(n):

            @pl.when(differs(src, first + origin))
            def _():
                part_arrival(src, part, count).wait_recv()

    def take(j):
        start = tile_of(twin, j) * LANES
        for src in range(n):
            for c in range(2):
                xt[src, c, pl.ds(pl.multiple_of(HALO + start, HALO), LANES), :] = lax.dot_general(
                    eye, raw[src, c, :, lanes(start)], NT, preferred_element_type=jnp.float32
                )

    def await_first(srcs):
        for src in srcs:

            @pl.when(differs(src, first + origin))
            def _():
                part_arrival(src, 0, parts[0][1]).wait_recv()

    inner_srcs = (half_size - 1, half_size)
    await_first(inner_srcs)

    @pl.when(holds)
    def _():
        send_middle()

    await_first([src for src in range(n) if src not in inner_srcs])
    take(0)

    await_signal(met, meets_right)
    halo_at = pl.ds(pl.multiple_of(twin * (block + HALO), HALO), HALO)
    ends = jnp.logical_or(at_left, at_right)

    @pl.when(jnp.logical_not(ends))
    def _():
        rim_copy().start()

    for part in range(max(1, len(parts) - 1), len(parts)):
        send_across(part)
        send_along(part)

    @pl.when(jnp.logical_not(ends))
    def _():
        rim_copy().wait()

    @pl.when(ends)
    def _():
        xt[:, :, halo_at, :] = jnp.zeros((n, 2, HALO, ANGLES), jnp.float32)

    def send_back(j, s, far):
        here = jnp.logical_and(s == me, origin == twin)
        for start, count in plans[far]:
            goes = jnp.logical_and(jnp.logical_not(here), j == start + count - 1)
            if far and start + count == tiles:
                goes = jnp.logical_and(goes, jnp.logical_or(mine == 0, s >= half_size))

            @pl.when(goes)
            def _():
                out_copy(start, count, s).start()

        @pl.when(here)
        def _():
            cols = tile_of(twin, j) * LANES
            out[:, mine, :, lanes(twin * block + cols)] = stage[s, :, :, lanes(cols)]

    def per_tile(j, carry):
        for part in range(1, len(parts)):

            @pl.when(j + 1 == parts[part][0])
            def _():
                await_part(part, parts[part][1])

        @pl.when(j < tiles - 1)
        def _():
            take(j + 1)

        @pl.when(j == tiles - 2)
        def _():
            twin_copy().start()

        @pl.when(j == tiles - 1)
        def _():
            twin_copy().wait()

        start = pl.multiple_of(tile_of(twin, j) * LANES, LANES)

        for level in range(LEVELS):
            mask = 2 ** (level % bits)
            base = RIM * level
            count = rows - 2 * base
            kept = count - 2 * RIM
            wide = kept + RIM

            pairs = [(p // mask * (2 * mask) + p % mask) for p in range(n // 2)]
            for pair, low in enumerate(pairs):
                members = (low, low + mask)
                for side in range(2):
                    k = shifts[level, side][None, :] + RIM
                    on8, on4, on2, on1 = [(k // p) % 2 == 1 for p in (8, 4, 2, 1)]
                    for c in range(2):
                        s = members[side]
                        b = side * 2 + c
                        held = xf.at[s, c] if level else xt.at[s, c, pl.ds(start, rows + 8)]
                        u = None
                        for t in range(TAPS):
                            term = taps[level, t] * held[pl.ds(base + t, count), :]
                            u = term if u is None else u + term
                        v = jnp.where(on8, u[RIM:], u[:wide])
                        sh0[b, :wide] = v
                        v = jnp.where(on4, sh0[b, pl.ds(4, wide), :], v)
                        sh1[b, :wide] = v
                        v = jnp.where(on2, sh1[b, pl.ds(2, wide), :], v)
                        sh2[b, :wide] = v
                        v = jnp.where(on1, sh2[b, pl.ds(1, kept), :], v[:kept])
                        i = b * ANGLES
                        ybuf[pair * kept : (pair + 1) * kept, i : i + ANGLES] = v.astype(jnp.bfloat16)
            y = ybuf[: n // 2 * kept, :]
            if level < LEVELS - 1:
                z = lax.dot_general(y, big[level], NT, preferred_element_type=jnp.float32)
                for pair, low in enumerate(pairs):
                    for half in range(2):
                        s = low + half * mask
                        i = half * 2 * ANGLES
                        r = pair * kept
                        re = z[r : r + kept, i : i + ANGLES]
                        im = z[r : r + kept, i + ANGLES : i + 2 * ANGLES]
                        span_rows = pl.ds(base + RIM, kept)
                        cosine = table[level, half, 0, span_rows, :]
                        sinus = table[level, half, 1, span_rows, :]
                        xf[s, 0, span_rows, :] = re * cosine - im * sinus
                        xf[s, 1, span_rows, :] = re * sinus + im * cosine
            else:
                z = lax.dot_general(big[level], y, NT, preferred_element_type=jnp.float32)
                for pair, low in enumerate(pairs):
                    for half in range(2):
                        s = low + half * mask
                        i = half * 2 * ANGLES
                        cosine, sinus = cols_table[half, 0], cols_table[half, 1]
                        r = pair * kept
                        re = z[i : i + ANGLES, r : r + kept]
                        im = z[i + ANGLES : i + 2 * ANGLES, r : r + kept]
                        stage[s, 0, :, lanes(start)] = (re * cosine - im * sinus).astype(jnp.bfloat16)
                        stage[s, 1, :, lanes(start)] = (re * sinus + im * cosine).astype(jnp.bfloat16)
                for group in (1 - mine, mine):
                    for spot_to in range(half_size):
                        send_back(j, group * half_size + spot_to, spot_to > 0)

            if level < LEVELS - 1:

                @pl.when(jnp.logical_and(at_left, j == 0))
                def _():
                    xf[:, :, :HALO, :] = jnp.zeros((n, 2, HALO, ANGLES), jnp.float32)

                @pl.when(jnp.logical_and(at_right, j == 0))
                def _():
                    xf[:, :, rows - HALO : rows, :] = jnp.zeros((n, 2, HALO, ANGLES), jnp.float32)

        return carry

    lax.fori_loop(0, tiles, per_tile, 0)

    @pl.when(mine == 1)
    def _():
        out_copy(*plans[0][-1], 0).wait_send()
        for z in range(1, half_size):
            out_copy(*plans[1][-1], z).start()

    for part in range(len(parts)):
        for core in range(CORES):
            part_copy(1 - mine, core, part).wait_send()

            @pl.when(differs(mine * half_size + home, first + core))
            def _():
                part_copy(mine, core, part).wait_send()

    for far, plan in enumerate(plans):
        for start, count in plan:
            for z in range(n):
                if (z % half_size > 0) == far:

                    waits = differs(z, first + origin)
                    if z == 0 and start + count == tiles:
                        waits = jnp.logical_and(waits, mine == 0)

                    @pl.when(waits)
                    def _():
                        out_copy(start, count, z).wait_send()

            for h in range(2):
                for core in range(CORES):
                    arrives = differs(h * half_size + home, first + core)

                    @pl.when(jnp.logical_and(arrives, (spot > 0) == far))
                    def _():
                        out_arrival(h, core, start, count).wait_recv()


def in_one_kernel(n, rngs, image, interp_weights, range_taps, range_shifts):
    width = image.shape[3]
    block = 2 * width // n
    tiles = block // LANES
    rows = LANES + 2 * HALO
    parts = len(tile_parts(tiles))
    rows_table, cols_table = phase_tables()
    vmem = pl.BlockSpec(memory_space=pltpu.VMEM)
    hbm = pl.BlockSpec(memory_space=pl.ANY)
    dma = pltpu.SemaphoreType.DMA
    f32, bf16 = jnp.float32, jnp.bfloat16
    return pl.pallas_call(
        functools.partial(merge_kernel, n, rngs),
        out_shape=pltpu.VMEM(image.shape, bf16),
        in_specs=[hbm] * 6,
        out_specs=vmem,
        scratch_shapes=[
            pltpu.VMEM(image.shape, bf16),
            pltpu.VMEM(interp_weights.shape, bf16),
            pltpu.SMEM(range_taps.shape, f32),
            pltpu.VMEM(range_shifts.shape, jnp.int32),
            pltpu.VMEM(rows_table.shape, f32),
            pltpu.VMEM(cols_table.shape, f32),
            dma((9,)),
            pltpu.VMEM((n, 2, ANGLES, block), bf16),
            pltpu.VMEM((n, 2, block + 2 * HALO + 8, ANGLES), f32),
            pltpu.VMEM((LEVELS, 4 * ANGLES, 4 * ANGLES), bf16),
            pltpu.VMEM((LEVELS - 1, 2, 2, rows, ANGLES), f32),
            pltpu.VMEM((n, 2, rows + 8, ANGLES), f32),
            pltpu.VMEM((4, rows + 8, ANGLES), f32),
            pltpu.VMEM((4, rows + 8, ANGLES), f32),
            pltpu.VMEM((4, rows + 8, ANGLES), f32),
            pltpu.VMEM((n // 2 * rows, 4 * ANGLES), bf16),
            pltpu.VMEM((n, 2, ANGLES, block), bf16),
            dma((2, CORES, parts)),
            dma((n, parts)),
            dma(()),
            dma(()),
            dma((tiles, n)),
            dma((2, CORES, tiles)),
            dma(()),
            dma(()),
            pltpu.SemaphoreType.REGULAR((n,)),
            pltpu.SemaphoreType.REGULAR,
        ],
        compiler_params=pltpu.CompilerParams(has_side_effects=True, collective_id=0),
    )(image, interp_weights, range_taps, range_shifts, rows_table, cols_table)


def fits_kernel(mesh, image_shape):
    n = mesh.shape["sub"]
    paired = mesh.shape["rng"] % CORES == 0
    tiled = image_shape[3] % (CORES * LANES) == 0 and image_shape[3] > CORES * LANES
    return paired and n == 2 * CORES and image_shape[1] == 2 and tiled and ANGLES == LANES


def per_device(mesh, image, *rest):
    if fits_kernel(mesh, image.shape):
        return in_one_kernel(mesh.shape["sub"], mesh.shape["rng"], image, *rest)
    return on_device(image, *rest)


def solution(mesh):
    return jax.shard_map(
        functools.partial(per_device, mesh),
        mesh=mesh,
        in_specs=(P(None, ("img", "sub"), None, "rng"), P(), P(), P()),
        out_specs=P(None, ("img", "sub"), None, "rng"),
        check_vma=False,
    )
```

```python
import math

import functools

import jax
import jax.numpy as jnp
import numpy as np
from jax import lax
from jax.experimental import pallas as pl
from jax.experimental.pallas import tpu as pltpu
from jax.sharding import PartitionSpec as P

ANGLES = 128
RANGE = 4096
RIM = 8
TAPS = 4
LEVELS = 4


phase_step = 2.0 * math.pi / 64.0


def padded_2(cells, sides, width):
    for axis, dim in sides:
        count = lax.axis_size(axis)
        ends = count - 1
        head = lax.slice_in_dim(cells, 0, width, axis=dim)
        tail = lax.slice_in_dim(cells, cells.shape[dim] - width, cells.shape[dim], axis=dim)
        cells = jnp.concatenate(
            [
                lax.ppermute(tail, axis, [(i, (i + 1) % count) for i in range(ends)]),
                cells,
                lax.ppermute(head, axis, [((i + 1) % count, i) for i in range(ends)]),
            ],
            axis=dim,
        )
    return cells


def from_partner(value, axis, stride):
    mask = 2**stride
    pairs = [(source, source ^ mask) for source in range(lax.axis_size(axis))]
    return lax.ppermute(value, axis, pairs)


def rotate(merged_sum, level_index, half_index, range_start, range_width):
    angle_rows = half_index * ANGLES + jnp.arange(ANGLES, dtype=jnp.int32)
    range_cols = range_start + jnp.arange(range_width, dtype=jnp.int32)
    wrapped = range_cols[None, :] * (angle_rows[:, None] + 1) * (7 + level_index) % 64
    phase = wrapped.astype(jnp.float32) * phase_step
    cosine = jnp.cos(phase)
    sinus = jnp.sin(phase)
    return jnp.stack(
        [
            merged_sum[0] * cosine - merged_sum[1] * sinus,
            merged_sum[0] * sinus + merged_sum[1] * cosine,
        ]
    )


def level_coef(range_taps, range_shifts, level_index, side_index):
    offsets = jnp.arange(2 * RIM + 1, dtype=jnp.int32) - RIM
    tap_ids = jnp.arange(TAPS, dtype=jnp.int32)
    hits = (
        range_shifts[level_index, side_index][:, None, None] + tap_ids[None, :, None]
        == offsets[None, None, :]
    )
    return jnp.einsum(
        "t,ato->ao",
        range_taps[level_index],
        hits.astype(jnp.float32),
        precision=lax.Precision.HIGHEST,
    )


def interpolate(padded, coef, range_width):
    total = None
    for offset_index in range(2 * RIM + 1):
        term = coef[:, offset_index, None] * padded[
            ..., offset_index : offset_index + range_width
        ].astype(jnp.float32)
        total = term if total is None else total + term
    return total.astype(jnp.bfloat16)


def block_of(weight_pair):
    return jnp.stack(
        [jnp.stack([weight_pair[0], -weight_pair[1]]), jnp.stack([weight_pair[1], weight_pair[0]])]
    )


def combine_sides(lower_rows, upper_rows, weights_level, half_index):
    chosen = lax.dynamic_index_in_dim(weights_level, half_index, 1, keepdims=False)
    merged_sum = None
    for side_index, source in ((0, lower_rows), (1, upper_rows)):
        product = jnp.einsum(
            "xcij,cgjr->xgir",
            block_of(chosen[side_index]),
            source,
            preferred_element_type=jnp.float32,
        )
        merged_sum = product if merged_sum is None else merged_sum + product
    return merged_sum


def on_device(image, interp_weights, range_taps, range_shifts):
    range_width = image.shape[3]
    sub_count = lax.axis_size("sub")
    bit_count = sub_count.bit_length() - 1
    sub_index = lax.axis_index("sub")
    range_start = lax.axis_index("rng") * range_width
    current = padded_2(image, (("rng", 3),), LEVELS * RIM)
    margin = LEVELS * RIM
    for level_index in range(LEVELS):
        bit = level_index % bit_count
        own_half = sub_index // 2**bit % 2
        padded = current
        margin = margin - RIM
        out_width = range_width + 2 * margin
        coef = jnp.where(
            own_half == 0,
            level_coef(range_taps, range_shifts, level_index, 0),
            level_coef(range_taps, range_shifts, level_index, 1),
        )
        own_rows = interpolate(padded, coef, out_width)
        partner = from_partner(own_rows, "sub", bit)
        lower_rows = jnp.where(own_half == 0, own_rows, partner)
        upper_rows = jnp.where(own_half == 0, partner, own_rows)
        merged = combine_sides(lower_rows, upper_rows, interp_weights[level_index], own_half)
        turned = rotate(merged, level_index, own_half, range_start - margin, out_width)
        global_cols = range_start - margin + jnp.arange(out_width, dtype=jnp.int32)
        inside = jnp.logical_and(global_cols >= 0, global_cols < RANGE)
        turned = jnp.where(inside, turned, 0.0)
        current = turned.astype(jnp.bfloat16)
    return current


PERIOD = 64
LANES = 128
CORES = 2
HALO = LEVELS * RIM
MESH = pl.DeviceIdType.MESH
NT = (((1,), (1,)), ((), ()))


def phase_tables():
    a = np.arange(ANGLES)
    tables = np.zeros((LEVELS, 2, 2, PERIOD, ANGLES), np.float32)
    for level in range(LEVELS):
        for half in range(2):
            start = -HALO if level < LEVELS - 1 else 0
            r = (start + np.arange(PERIOD))[:, None]
            wrapped = (r * (half * ANGLES + a + 1)[None, :] * (7 + level)) % PERIOD
            phase = wrapped * phase_step
            tables[level, half, 0] = np.cos(phase)
            tables[level, half, 1] = np.sin(phase)
    last = np.swapaxes(tables[LEVELS - 1], -1, -2)
    last = np.concatenate([last] * (LANES // PERIOD), -1)
    return tables[: LEVELS - 1], last


def tile_parts(tiles):
    return [(0, 2), *[(j, 1) for j in range(2, tiles)]]


def merge_kernel(
    n, rngs, image_hbm, weights_hbm, taps_hbm, shifts_hbm, rows_hbm, cols_hbm, out,
    image, weights, taps, shifts, rows_table, cols_table, load_sem,
    raw, xt, big, table, xf, sh0, sh1, sh2, ybuf, stage,
    tile_send, tile_recv, twin_send, twin_recv, out_send, out_recv,
    rim_send, rim_recv, seen, met,
):
    me = lax.axis_index("sub")
    place = lax.axis_index("rng")
    width = image_hbm.shape[3]
    half_size = n // 2
    block = 2 * width // n
    tiles = block // LANES
    rows = LANES + 2 * HALO
    bits = n.bit_length() - 1
    pairs = [(j, min(2, tiles - j)) for j in range(0, tiles, 2)]
    parts = tile_parts(tiles)
    plans = ([(j, 1) for j in range(tiles)], [*[(j, 1) for j in range(pairs[-1][0])], pairs[-1]])

    twin = place % CORES
    first = place - twin
    mine = me // half_size
    spot = me % half_size
    flip = place // CORES % 2
    home = twin + flip * (1 - 2 * twin)
    origin = spot + flip * (1 - 2 * spot)
    inner = twin != origin
    at_left = jnp.logical_and(place == 0, origin == 0)
    at_right = jnp.logical_and(place == rngs - 1, origin == CORES - 1)
    meets = jnp.logical_not(jnp.logical_or(inner, jnp.logical_or(at_left, at_right)))
    meets_right = jnp.logical_and(meets, twin == 1)
    meets_left = jnp.logical_and(meets, twin == 0)
    across = 1 - 2 * twin
    rim_sub = jnp.where(inner, mine * half_size + half_size - 1 - spot, me)
    rim_rng = jnp.where(inner, place + across, place - across)

    def tile_of(core, j):
        return j + core * (tiles - 1 - 2 * j)

    def lanes(start, count=1):
        return pl.ds(pl.multiple_of(start, LANES), count * LANES)

    def columns(core, j, count=1):
        return tile_of(core, j) * LANES - core * (count - 1) * LANES

    def part_copy(m, core, part, source=None):
        j, count = parts[part]
        start = columns(core, j, count)
        return pltpu.make_async_remote_copy(
            src_ref=(image if source is None else source).at[:, m, :, lanes(core * block + start, count)],
            dst_ref=raw.at[me, :, :, lanes(start, count)],
            send_sem=tile_send.at[m, core, part],
            recv_sem=tile_recv.at[me, part],
            device_id={"sub": m * half_size + home, "rng": first + core},
            device_id_type=MESH,
        )

    def part_arrival(src, part, count):
        here = raw.at[src, :, :, lanes(0, count)]
        return pltpu.make_async_remote_copy(
            src_ref=here,
            dst_ref=here,
            send_sem=tile_send.at[0, 0, 0],
            recv_sem=tile_recv.at[src, part],
            device_id={"sub": src, "rng": first + origin},
            device_id_type=MESH,
        )

    def rim_copy():
        return pltpu.make_async_remote_copy(
            src_ref=xt.at[:, :, pl.ds(pl.multiple_of(HALO + twin * (block - HALO), HALO), HALO), :],
            dst_ref=xt.at[
                :, :, pl.ds(pl.multiple_of((1 - twin) * (block + HALO), HALO), HALO), :
            ],
            send_sem=rim_send,
            recv_sem=rim_recv,
            device_id={"sub": rim_sub, "rng": rim_rng},
            device_id_type=MESH,
        )

    def twin_copy():
        return pltpu.make_async_remote_copy(
            src_ref=xt.at[:, :, pl.ds(pl.multiple_of(block - twin * (block - HALO), HALO), HALO), :],
            dst_ref=xt.at[:, :, pl.ds(pl.multiple_of(twin * (block + HALO), HALO), HALO), :],
            send_sem=twin_send,
            recv_sem=twin_recv,
            device_id={"rng": place + 1 - 2 * twin},
            device_id_type=MESH,
        )

    def out_copy(j, count, z):
        start = columns(twin, j, count)
        return pltpu.make_async_remote_copy(
            src_ref=stage.at[z, :, :, lanes(start, count)],
            dst_ref=out.at[:, mine, :, lanes(twin * block + start, count)],
            send_sem=out_send.at[j, z],
            recv_sem=out_recv.at[mine, twin, j],
            device_id={"sub": z, "rng": first + origin},
            device_id_type=MESH,
        )

    def out_arrival(h, core, j, count):
        here = out.at[:, h, :, lanes(core * block + columns(core, j, count), count)]
        return pltpu.make_async_remote_copy(
            src_ref=here,
            dst_ref=here,
            send_sem=out_send.at[0, 0],
            recv_sem=out_recv.at[h, core, j],
            device_id={"sub": h * half_size + home, "rng": first + core},
            device_id_type=MESH,
        )

    def differs(z, r):
        return jnp.logical_or(me != z, place != r)

    def signal(sem, cond, z, r):
        @pl.when(cond)
        def _():
            pl.semaphore_signal(sem, inc=1, device_id={"sub": z, "rng": r}, device_id_type=MESH)

    def await_signal(sem, cond, count=1):
        @pl.when(cond)
        def _():
            pl.semaphore_wait(sem, count)

    def load(k, m, start, size):
        cols = pl.ds(start, size)
        return pltpu.make_async_copy(image_hbm.at[:, m, :, cols], image.at[:, m, :, cols], load_sem.at[k])

    loads = [
        load(0, 1 - mine, 0, 2 * LANES),
        load(1, 1 - mine, width - 2 * LANES, 2 * LANES),
        load(2, mine, 0, width),
    ]
    if width > 4 * LANES:
        loads.append(load(3, 1 - mine, 2 * LANES, width - 4 * LANES))
    others = [
        pltpu.make_async_copy(src, dst, load_sem.at[4 + k])
        for k, (src, dst) in enumerate(
            (
                (weights_hbm, weights),
                (rows_hbm, rows_table),
                (cols_hbm, cols_table),
                (taps_hbm, taps),
                (shifts_hbm, shifts),
            )
        )
    ]
    for copy in loads[:2]:
        copy.start()

    barrier = pltpu.get_barrier_semaphore()
    for step in range(1, n):
        for c in range(CORES):
            signal(barrier, me + step < n, me + step, first + c)
    pl.semaphore_signal(
        barrier, inc=1, device_id={"rng": place + across}, device_id_type=MESH
    )
    signal(barrier, meets_right, me, place + 1)

    def send_across(part):
        for core in range(CORES):
            part_copy(1 - mine, core, part).start()

    def send_along(part):
        for core in range(CORES):

            @pl.when(differs(mine * half_size + home, first + core))
            def _():
                part_copy(mine, core, part).start()

    pl.semaphore_wait(barrier, 1 + CORES * me + meets_left.astype(jnp.int32))
    for step in range(1, n):
        for c in range(CORES):
            signal(seen.at[step], me - step >= 0, me - step, first + c)
    signal(met, meets_left, me, place - 1)

    @pl.when(mine == 1)
    def _():
        for core in range(CORES):
            part_copy(1 - mine, core, 0, image_hbm).start()

    for copy in loads[2:] + others:
        copy.start()
    loads[0].wait()
    loads[1].wait()

    loads[2].wait()

    @pl.when(home <= spot)
    def _():
        send_along(0)

    for copy in loads[3:]:
        copy.wait()
    for step in range(1, n):
        await_signal(seen.at[step], me + step < n, CORES)

        @pl.when(jnp.logical_and(mine == 0, half_size + home - me == step))
        def _():
            send_across(0)

        if step == 1:

            @pl.when(home > spot)
            def _():
                send_along(0)

    def unit(count, shift):
        i = lax.broadcasted_iota(jnp.int32, (count, LANES), 0)
        k = lax.broadcasted_iota(jnp.int32, (count, LANES), 1)
        return (i + shift == k).astype(jnp.bfloat16)

    holds = me == half_size - 1

    def send_middle():
        for part in range(1, len(parts) - 1):
            send_across(part)
            send_along(part)

    @pl.when(jnp.logical_not(holds))
    def _():
        send_middle()

    for copy in others:
        copy.wait()

    for level in range(LEVELS):
        for half in range(2):
            for side in range(2):
                real = weights[level, side, half, 0]
                imag = weights[level, side, half, 1]
                i = half * 2 * ANGLES
                j = side * 2 * ANGLES
                big[level, i : i + ANGLES, j : j + ANGLES] = real
                big[level, i : i + ANGLES, j + ANGLES : j + 2 * ANGLES] = -imag
                big[level, i + ANGLES : i + 2 * ANGLES, j : j + ANGLES] = imag
                big[level, i + ANGLES : i + 2 * ANGLES, j + ANGLES : j + 2 * ANGLES] = real
            if level < LEVELS - 1:
                for part in range(2):
                    for start in range(0, rows, PERIOD):
                        size = min(PERIOD, rows - start)
                        table[level, half, part, start : start + size, :] = rows_table[
                            level, half, part, :size, :
                        ]

    eye = unit(LANES, 0)

    @pl.when(twin == origin)
    def _():
        raw[me] = image[:, mine, :, lanes(twin * block, tiles)]

    def await_part(part, count):
        for src in range(n):

            @pl.when(differs(src, first + origin))
            def _():
                part_arrival(src, part, count).wait_recv()

    def take(j):
        start = tile_of(twin, j) * LANES
        for src in range(n):
            for c in range(2):
                xt[src, c, pl.ds(pl.multiple_of(HALO + start, HALO), LANES), :] = lax.dot_general(
                    eye, raw[src, c, :, lanes(start)], NT, preferred_element_type=jnp.float32
                )

    def await_first(srcs):
        for src in srcs:

            @pl.when(differs(src, first + origin))
            def _():
                part_arrival(src, 0, parts[0][1]).wait_recv()

    inner_srcs = (half_size,)
    await_first(inner_srcs)

    @pl.when(holds)
    def _():
        send_middle()

    await_first([src for src in range(n) if src not in inner_srcs])
    take(0)

    await_signal(met, meets_right)
    halo_at = pl.ds(pl.multiple_of(twin * (block + HALO), HALO), HALO)
    ends = jnp.logical_or(at_left, at_right)

    @pl.when(jnp.logical_not(ends))
    def _():
        rim_copy().start()

    for part in range(max(1, len(parts) - 1), len(parts)):
        send_across(part)
        send_along(part)

    @pl.when(jnp.logical_not(ends))
    def _():
        rim_copy().wait()

    @pl.when(ends)
    def _():
        xt[:, :, halo_at, :] = jnp.zeros((n, 2, HALO, ANGLES), jnp.float32)

    def send_back(j, s, far):
        here = jnp.logical_and(s == me, origin == twin)
        for start, count in plans[far]:
            goes = jnp.logical_and(jnp.logical_not(here), j == start + count - 1)
            if far and start + count == tiles:
                goes = jnp.logical_and(goes, jnp.logical_or(mine == 0, s >= half_size))

            @pl.when(goes)
            def _():
                out_copy(start, count, s).start()

        @pl.when(here)
        def _():
            cols = tile_of(twin, j) * LANES
            out[:, mine, :, lanes(twin * block + cols)] = stage[s, :, :, lanes(cols)]

    def per_tile(j, carry):
        for part in range(1, len(parts)):

            @pl.when(j + 1 == parts[part][0])
            def _():
                await_part(part, parts[part][1])

        @pl.when(j < tiles - 1)
        def _():
            take(j + 1)

        @pl.when(j == tiles - 2)
        def _():
            twin_copy().start()

        @pl.when(j == tiles - 1)
        def _():
            twin_copy().wait()

        start = pl.multiple_of(tile_of(twin, j) * LANES, LANES)

        for level in range(LEVELS):
            mask = 2 ** (level % bits)
            base = RIM * level
            count = rows - 2 * base
            kept = count - 2 * RIM
            wide = kept + RIM

            pairs = [(p // mask * (2 * mask) + p % mask) for p in range(n // 2)]
            for pair, low in enumerate(pairs):
                members = (low, low + mask)
                for side in range(2):
                    k = shifts[level, side][None, :] + RIM
                    on8, on4, on2, on1 = [(k // p) % 2 == 1 for p in (8, 4, 2, 1)]
                    for c in range(2):
                        s = members[side]
                        b = side * 2 + c
                        held = xf.at[s, c] if level else xt.at[s, c, pl.ds(start, rows + 8)]
                        u = None
                        for t in range(TAPS):
                            term = taps[level, t] * held[pl.ds(base + t, count), :]
                            u = term if u is None else u + term
                        v = jnp.where(on8, u[RIM:], u[:wide])
                        sh0[b, :wide] = v
                        v = jnp.where(on4, sh0[b, pl.ds(4, wide), :], v)
                        sh1[b, :wide] = v
                        v = jnp.where(on2, sh1[b, pl.ds(2, wide), :], v)
                        sh2[b, :wide] = v
                        v = jnp.where(on1, sh2[b, pl.ds(1, kept), :], v[:kept])
                        i = b * ANGLES
                        ybuf[pair * kept : (pair + 1) * kept, i : i + ANGLES] = v.astype(jnp.bfloat16)
            y = ybuf[: n // 2 * kept, :]
            if level < LEVELS - 1:
                z = lax.dot_general(y, big[level], NT, preferred_element_type=jnp.float32)
                for pair, low in enumerate(pairs):
                    for half in range(2):
                        s = low + half * mask
                        i = half * 2 * ANGLES
                        r = pair * kept
                        re = z[r : r + kept, i : i + ANGLES]
                        im = z[r : r + kept, i + ANGLES : i + 2 * ANGLES]
                        span_rows = pl.ds(base + RIM, kept)
                        cosine = table[level, half, 0, span_rows, :]
                        sinus = table[level, half, 1, span_rows, :]
                        xf[s, 0, span_rows, :] = re * cosine - im * sinus
                        xf[s, 1, span_rows, :] = re * sinus + im * cosine
            else:
                z = lax.dot_general(big[level], y, NT, preferred_element_type=jnp.float32)
                for pair, low in enumerate(pairs):
                    for half in range(2):
                        s = low + half * mask
                        i = half * 2 * ANGLES
                        cosine, sinus = cols_table[half, 0], cols_table[half, 1]
                        r = pair * kept
                        re = z[i : i + ANGLES, r : r + kept]
                        im = z[i + ANGLES : i + 2 * ANGLES, r : r + kept]
                        stage[s, 0, :, lanes(start)] = (re * cosine - im * sinus).astype(jnp.bfloat16)
                        stage[s, 1, :, lanes(start)] = (re * sinus + im * cosine).astype(jnp.bfloat16)
                for group in (1 - mine, mine):
                    for spot_to in range(half_size):
                        send_back(j, group * half_size + spot_to, spot_to > 0)

            if level < LEVELS - 1:

                @pl.when(jnp.logical_and(at_left, j == 0))
                def _():
                    xf[:, :, :HALO, :] = jnp.zeros((n, 2, HALO, ANGLES), jnp.float32)

                @pl.when(jnp.logical_and(at_right, j == 0))
                def _():
                    xf[:, :, rows - HALO : rows, :] = jnp.zeros((n, 2, HALO, ANGLES), jnp.float32)

        return carry

    lax.fori_loop(0, tiles, per_tile, 0)

    @pl.when(mine == 1)
    def _():
        out_copy(*plans[0][-1], 0).wait_send()
        for z in range(1, half_size):
            out_copy(*plans[1][-1], z).start()

    for part in range(len(parts)):
        for core in range(CORES):
            part_copy(1 - mine, core, part).wait_send()

            @pl.when(differs(mine * half_size + home, first + core))
            def _():
                part_copy(mine, core, part).wait_send()

    for far, plan in enumerate(plans):
        for start, count in plan:
            for z in range(n):
                if (z % half_size > 0) == far:

                    waits = differs(z, first + origin)
                    if z == 0 and start + count == tiles:
                        waits = jnp.logical_and(waits, mine == 0)

                    @pl.when(waits)
                    def _():
                        out_copy(start, count, z).wait_send()

            for h in range(2):
                for core in range(CORES):
                    arrives = differs(h * half_size + home, first + core)

                    @pl.when(jnp.logical_and(arrives, (spot > 0) == far))
                    def _():
                        out_arrival(h, core, start, count).wait_recv()


def in_one_kernel(n, rngs, image, interp_weights, range_taps, range_shifts):
    width = image.shape[3]
    block = 2 * width // n
    tiles = block // LANES
    rows = LANES + 2 * HALO
    parts = len(tile_parts(tiles))
    rows_table, cols_table = phase_tables()
    vmem = pl.BlockSpec(memory_space=pltpu.VMEM)
    hbm = pl.BlockSpec(memory_space=pl.ANY)
    dma = pltpu.SemaphoreType.DMA
    f32, bf16 = jnp.float32, jnp.bfloat16
    return pl.pallas_call(
        functools.partial(merge_kernel, n, rngs),
        out_shape=pltpu.VMEM(image.shape, bf16),
        in_specs=[hbm] * 6,
        out_specs=vmem,
        scratch_shapes=[
            pltpu.VMEM(image.shape, bf16),
            pltpu.VMEM(interp_weights.shape, bf16),
            pltpu.SMEM(range_taps.shape, f32),
            pltpu.VMEM(range_shifts.shape, jnp.int32),
            pltpu.VMEM(rows_table.shape, f32),
            pltpu.VMEM(cols_table.shape, f32),
            dma((9,)),
            pltpu.VMEM((n, 2, ANGLES, block), bf16),
            pltpu.VMEM((n, 2, block + 2 * HALO + 8, ANGLES), f32),
            pltpu.VMEM((LEVELS, 4 * ANGLES, 4 * ANGLES), bf16),
            pltpu.VMEM((LEVELS - 1, 2, 2, rows, ANGLES), f32),
            pltpu.VMEM((n, 2, rows + 8, ANGLES), f32),
            pltpu.VMEM((4, rows + 8, ANGLES), f32),
            pltpu.VMEM((4, rows + 8, ANGLES), f32),
            pltpu.VMEM((4, rows + 8, ANGLES), f32),
            pltpu.VMEM((n // 2 * rows, 4 * ANGLES), bf16),
            pltpu.VMEM((n, 2, ANGLES, block), bf16),
            dma((2, CORES, parts)),
            dma((n, parts)),
            dma(()),
            dma(()),
            dma((tiles, n)),
            dma((2, CORES, tiles)),
            dma(()),
            dma(()),
            pltpu.SemaphoreType.REGULAR((n,)),
            pltpu.SemaphoreType.REGULAR,
        ],
        compiler_params=pltpu.CompilerParams(has_side_effects=True, collective_id=0),
    )(image, interp_weights, range_taps, range_shifts, rows_table, cols_table)


def fits_kernel(mesh, image_shape):
    n = mesh.shape["sub"]
    paired = mesh.shape["rng"] % CORES == 0
    tiled = image_shape[3] % (CORES * LANES) == 0 and image_shape[3] > CORES * LANES
    return paired and n == 2 * CORES and image_shape[1] == 2 and tiled and ANGLES == LANES


def per_device(mesh, image, *rest):
    if fits_kernel(mesh, image.shape):
        return in_one_kernel(mesh.shape["sub"], mesh.shape["rng"], image, *rest)
    return on_device(image, *rest)


def solution(mesh):
    return jax.shard_map(
        functools.partial(per_device, mesh),
        mesh=mesh,
        in_specs=(P(None, ("img", "sub"), None, "rng"), P(), P(), P()),
        out_specs=P(None, ("img", "sub"), None, "rng"),
        check_vma=False,
    )
```

```python
import math

import functools

import jax
import jax.numpy as jnp
import numpy as np
from jax import lax
from jax.experimental import pallas as pl
from jax.experimental.pallas import tpu as pltpu
from jax.sharding import PartitionSpec as P

ANGLES = 128
RANGE = 4096
RIM = 8
TAPS = 4
LEVELS = 4


phase_step = 2.0 * math.pi / 64.0


def padded_2(cells, sides, width):
    for axis, dim in sides:
        count = lax.axis_size(axis)
        ends = count - 1
        head = lax.slice_in_dim(cells, 0, width, axis=dim)
        tail = lax.slice_in_dim(cells, cells.shape[dim] - width, cells.shape[dim], axis=dim)
        cells = jnp.concatenate(
            [
                lax.ppermute(tail, axis, [(i, (i + 1) % count) for i in range(ends)]),
                cells,
                lax.ppermute(head, axis, [((i + 1) % count, i) for i in range(ends)]),
            ],
            axis=dim,
        )
    return cells


def from_partner(value, axis, stride):
    mask = 2**stride
    pairs = [(source, source ^ mask) for source in range(lax.axis_size(axis))]
    return lax.ppermute(value, axis, pairs)


def rotate(merged_sum, level_index, half_index, range_start, range_width):
    angle_rows = half_index * ANGLES + jnp.arange(ANGLES, dtype=jnp.int32)
    range_cols = range_start + jnp.arange(range_width, dtype=jnp.int32)
    wrapped = range_cols[None, :] * (angle_rows[:, None] + 1) * (7 + level_index) % 64
    phase = wrapped.astype(jnp.float32) * phase_step
    cosine = jnp.cos(phase)
    sinus = jnp.sin(phase)
    return jnp.stack(
        [
            merged_sum[0] * cosine - merged_sum[1] * sinus,
            merged_sum[0] * sinus + merged_sum[1] * cosine,
        ]
    )


def level_coef(range_taps, range_shifts, level_index, side_index):
    offsets = jnp.arange(2 * RIM + 1, dtype=jnp.int32) - RIM
    tap_ids = jnp.arange(TAPS, dtype=jnp.int32)
    hits = (
        range_shifts[level_index, side_index][:, None, None] + tap_ids[None, :, None]
        == offsets[None, None, :]
    )
    return jnp.einsum(
        "t,ato->ao",
        range_taps[level_index],
        hits.astype(jnp.float32),
        precision=lax.Precision.HIGHEST,
    )


def interpolate(padded, coef, range_width):
    total = None
    for offset_index in range(2 * RIM + 1):
        term = coef[:, offset_index, None] * padded[
            ..., offset_index : offset_index + range_width
        ].astype(jnp.float32)
        total = term if total is None else total + term
    return total.astype(jnp.bfloat16)


def block_of(weight_pair):
    return jnp.stack(
        [jnp.stack([weight_pair[0], -weight_pair[1]]), jnp.stack([weight_pair[1], weight_pair[0]])]
    )


def combine_sides(lower_rows, upper_rows, weights_level, half_index):
    chosen = lax.dynamic_index_in_dim(weights_level, half_index, 1, keepdims=False)
    merged_sum = None
    for side_index, source in ((0, lower_rows), (1, upper_rows)):
        product = jnp.einsum(
            "xcij,cgjr->xgir",
            block_of(chosen[side_index]),
            source,
            preferred_element_type=jnp.float32,
        )
        merged_sum = product if merged_sum is None else merged_sum + product
    return merged_sum


def on_device(image, interp_weights, range_taps, range_shifts):
    range_width = image.shape[3]
    sub_count = lax.axis_size("sub")
    bit_count = sub_count.bit_length() - 1
    sub_index = lax.axis_index("sub")
    range_start = lax.axis_index("rng") * range_width
    current = padded_2(image, (("rng", 3),), LEVELS * RIM)
    margin = LEVELS * RIM
    for level_index in range(LEVELS):
        bit = level_index % bit_count
        own_half = sub_index // 2**bit % 2
        padded = current
        margin = margin - RIM
        out_width = range_width + 2 * margin
        coef = jnp.where(
            own_half == 0,
            level_coef(range_taps, range_shifts, level_index, 0),
            level_coef(range_taps, range_shifts, level_index, 1),
        )
        own_rows = interpolate(padded, coef, out_width)
        partner = from_partner(own_rows, "sub", bit)
        lower_rows = jnp.where(own_half == 0, own_rows, partner)
        upper_rows = jnp.where(own_half == 0, partner, own_rows)
        merged = combine_sides(lower_rows, upper_rows, interp_weights[level_index], own_half)
        turned = rotate(merged, level_index, own_half, range_start - margin, out_width)
        global_cols = range_start - margin + jnp.arange(out_width, dtype=jnp.int32)
        inside = jnp.logical_and(global_cols >= 0, global_cols < RANGE)
        turned = jnp.where(inside, turned, 0.0)
        current = turned.astype(jnp.bfloat16)
    return current


PERIOD = 64
LANES = 128
CORES = 2
HALO = LEVELS * RIM
MESH = pl.DeviceIdType.MESH
NT = (((1,), (1,)), ((), ()))


def phase_tables():
    a = np.arange(ANGLES)
    tables = np.zeros((LEVELS, 2, 2, PERIOD, ANGLES), np.float32)
    for level in range(LEVELS):
        for half in range(2):
            start = -HALO if level < LEVELS - 1 else 0
            r = (start + np.arange(PERIOD))[:, None]
            wrapped = (r * (half * ANGLES + a + 1)[None, :] * (7 + level)) % PERIOD
            phase = wrapped * phase_step
            tables[level, half, 0] = np.cos(phase)
            tables[level, half, 1] = np.sin(phase)
    last = np.swapaxes(tables[LEVELS - 1], -1, -2)
    last = np.concatenate([last] * (LANES // PERIOD), -1)
    return tables[: LEVELS - 1], last


def tile_parts(tiles):
    return [(0, 2), *[(j, 1) for j in range(2, tiles)]]


def merge_kernel(
    n, rngs, image_hbm, weights_hbm, taps_hbm, shifts_hbm, rows_hbm, cols_hbm, out,
    image, weights, taps, shifts, rows_table, cols_table, load_sem,
    raw, xt, rim_out, rim_in, big, table, xf, sh0, sh1, sh2, ybuf, stage,
    tile_send, tile_recv, twin_send, twin_recv, out_send, out_recv,
    rim_send, rim_recv, seen, met,
):
    me = lax.axis_index("sub")
    place = lax.axis_index("rng")
    width = image_hbm.shape[3]
    half_size = n // 2
    block = 2 * width // n
    tiles = block // LANES
    rows = LANES + 2 * HALO
    bits = n.bit_length() - 1
    pairs = [(j, min(2, tiles - j)) for j in range(0, tiles, 2)]
    parts = tile_parts(tiles)
    plans = ([(j, 1) for j in range(tiles)], [*[(j, 1) for j in range(pairs[-1][0])], pairs[-1]])

    twin = place % CORES
    first = place - twin
    mine = me // half_size
    spot = me % half_size
    flip = place // CORES % 2
    home = twin + flip * (1 - 2 * twin)
    origin = spot + flip * (1 - 2 * spot)
    inner = twin != origin
    at_left = jnp.logical_and(place == 0, origin == 0)
    at_right = jnp.logical_and(place == rngs - 1, origin == CORES - 1)
    meets = jnp.logical_not(jnp.logical_or(inner, jnp.logical_or(at_left, at_right)))
    meets_right = jnp.logical_and(meets, twin == 1)
    meets_left = jnp.logical_and(meets, twin == 0)
    across = 1 - 2 * twin
    rim_sub = jnp.where(inner, mine * half_size + half_size - 1 - spot, me)
    rim_rng = jnp.where(inner, place + across, place - across)

    def tile_of(core, j):
        return j + core * (tiles - 1 - 2 * j)

    def lanes(start, count=1):
        return pl.ds(pl.multiple_of(start, LANES), count * LANES)

    def columns(core, j, count=1):
        return tile_of(core, j) * LANES - core * (count - 1) * LANES

    def part_copy(m, core, part, source=None):
        j, count = parts[part]
        start = columns(core, j, count)
        return pltpu.make_async_remote_copy(
            src_ref=(image if source is None else source).at[:, m, :, lanes(core * block + start, count)],
            dst_ref=raw.at[me, :, :, lanes(start, count)],
            send_sem=tile_send.at[m, core, part],
            recv_sem=tile_recv.at[me, part],
            device_id={"sub": m * half_size + home, "rng": first + core},
            device_id_type=MESH,
        )

    def part_arrival(src, part, count):
        here = raw.at[src, :, :, lanes(0, count)]
        return pltpu.make_async_remote_copy(
            src_ref=here,
            dst_ref=here,
            send_sem=tile_send.at[0, 0, 0],
            recv_sem=tile_recv.at[src, part],
            device_id={"sub": src, "rng": first + origin},
            device_id_type=MESH,
        )

    def rim_copy():
        return pltpu.make_async_remote_copy(
            src_ref=rim_out,
            dst_ref=rim_in,
            send_sem=rim_send,
            recv_sem=rim_recv,
            device_id={"sub": rim_sub, "rng": rim_rng},
            device_id_type=MESH,
        )

    def twin_copy():
        return pltpu.make_async_remote_copy(
            src_ref=xt.at[:, :, pl.ds(pl.multiple_of(block - twin * (block - HALO), HALO), HALO), :],
            dst_ref=xt.at[:, :, pl.ds(pl.multiple_of(twin * (block + HALO), HALO), HALO), :],
            send_sem=twin_send,
            recv_sem=twin_recv,
            device_id={"rng": place + 1 - 2 * twin},
            device_id_type=MESH,
        )

    def out_copy(j, count, z):
        start = columns(twin, j, count)
        return pltpu.make_async_remote_copy(
            src_ref=stage.at[z, :, :, lanes(start, count)],
            dst_ref=out.at[:, mine, :, lanes(twin * block + start, count)],
            send_sem=out_send.at[j, z],
            recv_sem=out_recv.at[mine, twin, j],
            device_id={"sub": z, "rng": first + origin},
            device_id_type=MESH,
        )

    def out_arrival(h, core, j, count):
        here = out.at[:, h, :, lanes(core * block + columns(core, j, count), count)]
        return pltpu.make_async_remote_copy(
            src_ref=here,
            dst_ref=here,
            send_sem=out_send.at[0, 0],
            recv_sem=out_recv.at[h, core, j],
            device_id={"sub": h * half_size + home, "rng": first + core},
            device_id_type=MESH,
        )

    def differs(z, r):
        return jnp.logical_or(me != z, place != r)

    def signal(sem, cond, z, r):
        @pl.when(cond)
        def _():
            pl.semaphore_signal(sem, inc=1, device_id={"sub": z, "rng": r}, device_id_type=MESH)

    def await_signal(sem, cond, count=1):
        @pl.when(cond)
        def _():
            pl.semaphore_wait(sem, count)

    def load(k, m, start, size):
        cols = pl.ds(start, size)
        return pltpu.make_async_copy(image_hbm.at[:, m, :, cols], image.at[:, m, :, cols], load_sem.at[k])

    loads = [
        load(0, 1 - mine, 0, 2 * LANES),
        load(1, 1 - mine, width - 2 * LANES, 2 * LANES),
        load(2, mine, 0, width),
    ]
    if width > 4 * LANES:
        loads.append(load(3, 1 - mine, 2 * LANES, width - 4 * LANES))
    others = [
        pltpu.make_async_copy(src, dst, load_sem.at[4 + k])
        for k, (src, dst) in enumerate(
            (
                (weights_hbm, weights),
                (rows_hbm, rows_table),
                (cols_hbm, cols_table),
                (taps_hbm, taps),
                (shifts_hbm, shifts),
            )
        )
    ]
    for copy in loads[:2]:
        copy.start()

    barrier = pltpu.get_barrier_semaphore()
    for step in range(1, n):
        for c in range(CORES):
            signal(barrier, me + step < n, me + step, first + c)
    pl.semaphore_signal(
        barrier, inc=1, device_id={"rng": place + across}, device_id_type=MESH
    )
    signal(barrier, meets_right, me, place + 1)

    def send_across(part):
        for core in range(CORES):
            part_copy(1 - mine, core, part).start()

    def send_along(part):
        for core in range(CORES):

            @pl.when(differs(mine * half_size + home, first + core))
            def _():
                part_copy(mine, core, part).start()

    pl.semaphore_wait(barrier, 1 + CORES * me + meets_left.astype(jnp.int32))
    for step in range(1, n):
        for c in range(CORES):
            signal(seen.at[step], me - step >= 0, me - step, first + c)
    signal(met, meets_left, me, place - 1)

    @pl.when(mine == 1)
    def _():
        for core in range(CORES):
            part_copy(1 - mine, core, 0, image_hbm).start()

    for copy in loads[2:] + others:
        copy.start()
    loads[0].wait()
    loads[1].wait()

    loads[2].wait()

    @pl.when(home <= spot)
    def _():
        send_along(0)

    for copy in loads[3:]:
        copy.wait()
    for step in range(1, n):
        await_signal(seen.at[step], me + step < n, CORES)

        @pl.when(jnp.logical_and(mine == 0, half_size + home - me == step))
        def _():
            send_across(0)

        if step == 1:

            @pl.when(home > spot)
            def _():
                send_along(0)

    def unit(count, shift):
        i = lax.broadcasted_iota(jnp.int32, (count, LANES), 0)
        k = lax.broadcasted_iota(jnp.int32, (count, LANES), 1)
        return (i + shift == k).astype(jnp.bfloat16)

    holds = me == half_size - 1

    def send_middle():
        for part in range(1, len(parts) - 1):
            send_across(part)
            send_along(part)

    @pl.when(jnp.logical_not(holds))
    def _():
        send_middle()

    for copy in others:
        copy.wait()

    for level in range(LEVELS):
        for half in range(2):
            for side in range(2):
                real = weights[level, side, half, 0]
                imag = weights[level, side, half, 1]
                i = half * 2 * ANGLES
                j = side * 2 * ANGLES
                big[level, i : i + ANGLES, j : j + ANGLES] = real
                big[level, i : i + ANGLES, j + ANGLES : j + 2 * ANGLES] = -imag
                big[level, i + ANGLES : i + 2 * ANGLES, j : j + ANGLES] = imag
                big[level, i + ANGLES : i + 2 * ANGLES, j + ANGLES : j + 2 * ANGLES] = real
            if level < LEVELS - 1:
                for part in range(2):
                    for start in range(0, rows, PERIOD):
                        size = min(PERIOD, rows - start)
                        table[level, half, part, start : start + size, :] = rows_table[
                            level, half, part, :size, :
                        ]

    eye = unit(LANES, 0)

    @pl.when(twin == origin)
    def _():
        raw[me] = image[:, mine, :, lanes(twin * block, tiles)]

    def await_part(part, count):
        for src in range(n):

            @pl.when(differs(src, first + origin))
            def _():
                part_arrival(src, part, count).wait_recv()

    def take(j):
        start = tile_of(twin, j) * LANES
        for src in range(n):
            for c in range(2):
                xt[src, c, pl.ds(pl.multiple_of(HALO + start, HALO), LANES), :] = lax.dot_general(
                    eye, raw[src, c, :, lanes(start)], NT, preferred_element_type=jnp.float32
                )

    def await_first(srcs):
        for src in srcs:

            @pl.when(differs(src, first + origin))
            def _():
                part_arrival(src, 0, parts[0][1]).wait_recv()

    inner_srcs = (half_size,)
    await_first(inner_srcs)

    @pl.when(holds)
    def _():
        send_middle()

    await_first([src for src in range(n) if src not in inner_srcs])
    take(0)

    await_signal(met, meets_right)
    halo_at = pl.ds(pl.multiple_of(twin * (block + HALO), HALO), HALO)
    ends = jnp.logical_or(at_left, at_right)

    @pl.when(jnp.logical_not(ends))
    def _():
        rim = pl.ds(pl.multiple_of(HALO + twin * (block - HALO), HALO), HALO)
        rim_out[...] = xt[:, :, rim, :].astype(jnp.bfloat16)
        rim_copy().start()

    for part in range(max(1, len(parts) - 1), len(parts)):
        send_across(part)
        send_along(part)

    @pl.when(jnp.logical_not(ends))
    def _():
        rim_copy().wait()
        xt[:, :, halo_at, :] = rim_in[...].astype(jnp.float32)

    @pl.when(ends)
    def _():
        xt[:, :, halo_at, :] = jnp.zeros((n, 2, HALO, ANGLES), jnp.float32)

    def send_back(j, s, far):
        here = jnp.logical_and(s == me, origin == twin)
        for start, count in plans[far]:
            goes = jnp.logical_and(jnp.logical_not(here), j == start + count - 1)
            if far and start + count == tiles:
                goes = jnp.logical_and(goes, jnp.logical_or(mine == 0, s >= half_size))

            @pl.when(goes)
            def _():
                out_copy(start, count, s).start()

        @pl.when(here)
        def _():
            cols = tile_of(twin, j) * LANES
            out[:, mine, :, lanes(twin * block + cols)] = stage[s, :, :, lanes(cols)]

    def per_tile(j, carry):
        for part in range(1, len(parts)):

            @pl.when(j + 1 == parts[part][0])
            def _():
                await_part(part, parts[part][1])

        @pl.when(j < tiles - 1)
        def _():
            take(j + 1)

        @pl.when(j == tiles - 2)
        def _():
            twin_copy().start()

        @pl.when(j == tiles - 1)
        def _():
            twin_copy().wait()

        start = pl.multiple_of(tile_of(twin, j) * LANES, LANES)

        for level in range(LEVELS):
            mask = 2 ** (level % bits)
            base = RIM * level
            count = rows - 2 * base
            kept = count - 2 * RIM
            wide = kept + RIM

            pairs = [(p // mask * (2 * mask) + p % mask) for p in range(n // 2)]
            for pair, low in enumerate(pairs):
                members = (low, low + mask)
                for side in range(2):
                    k = shifts[level, side][None, :] + RIM
                    on8, on4, on2, on1 = [(k // p) % 2 == 1 for p in (8, 4, 2, 1)]
                    for c in range(2):
                        s = members[side]
                        b = side * 2 + c
                        held = xf.at[s, c] if level else xt.at[s, c, pl.ds(start, rows + 8)]
                        u = None
                        for t in range(TAPS):
                            term = taps[level, t] * held[pl.ds(base + t, count), :]
                            u = term if u is None else u + term
                        v = jnp.where(on8, u[RIM:], u[:wide])
                        sh0[b, :wide] = v
                        v = jnp.where(on4, sh0[b, pl.ds(4, wide), :], v)
                        sh1[b, :wide] = v
                        v = jnp.where(on2, sh1[b, pl.ds(2, wide), :], v)
                        sh2[b, :wide] = v
                        v = jnp.where(on1, sh2[b, pl.ds(1, kept), :], v[:kept])
                        i = b * ANGLES
                        ybuf[pair * kept : (pair + 1) * kept, i : i + ANGLES] = v.astype(jnp.bfloat16)
            y = ybuf[: n // 2 * kept, :]
            if level < LEVELS - 1:
                z = lax.dot_general(y, big[level], NT, preferred_element_type=jnp.float32)
                for pair, low in enumerate(pairs):
                    for half in range(2):
                        s = low + half * mask
                        i = half * 2 * ANGLES
                        r = pair * kept
                        re = z[r : r + kept, i : i + ANGLES]
                        im = z[r : r + kept, i + ANGLES : i + 2 * ANGLES]
                        span_rows = pl.ds(base + RIM, kept)
                        cosine = table[level, half, 0, span_rows, :]
                        sinus = table[level, half, 1, span_rows, :]
                        xf[s, 0, span_rows, :] = re * cosine - im * sinus
                        xf[s, 1, span_rows, :] = re * sinus + im * cosine
            else:
                z = lax.dot_general(big[level], y, NT, preferred_element_type=jnp.float32)
                for pair, low in enumerate(pairs):
                    for half in range(2):
                        s = low + half * mask
                        i = half * 2 * ANGLES
                        cosine, sinus = cols_table[half, 0], cols_table[half, 1]
                        r = pair * kept
                        re = z[i : i + ANGLES, r : r + kept]
                        im = z[i + ANGLES : i + 2 * ANGLES, r : r + kept]
                        stage[s, 0, :, lanes(start)] = (re * cosine - im * sinus).astype(jnp.bfloat16)
                        stage[s, 1, :, lanes(start)] = (re * sinus + im * cosine).astype(jnp.bfloat16)
                for group in (1 - mine, mine):
                    for spot_to in range(half_size):
                        send_back(j, group * half_size + spot_to, spot_to > 0)

            if level < LEVELS - 1:

                @pl.when(jnp.logical_and(at_left, j == 0))
                def _():
                    xf[:, :, :HALO, :] = jnp.zeros((n, 2, HALO, ANGLES), jnp.float32)

                @pl.when(jnp.logical_and(at_right, j == 0))
                def _():
                    xf[:, :, rows - HALO : rows, :] = jnp.zeros((n, 2, HALO, ANGLES), jnp.float32)

        return carry

    lax.fori_loop(0, tiles, per_tile, 0)

    @pl.when(mine == 1)
    def _():
        out_copy(*plans[0][-1], 0).wait_send()
        for z in range(1, half_size):
            out_copy(*plans[1][-1], z).start()

    for part in range(len(parts)):
        for core in range(CORES):
            part_copy(1 - mine, core, part).wait_send()

            @pl.when(differs(mine * half_size + home, first + core))
            def _():
                part_copy(mine, core, part).wait_send()

    for far, plan in enumerate(plans):
        for start, count in plan:
            for z in range(n):
                if (z % half_size > 0) == far:

                    waits = differs(z, first + origin)
                    if z == 0 and start + count == tiles:
                        waits = jnp.logical_and(waits, mine == 0)

                    @pl.when(waits)
                    def _():
                        out_copy(start, count, z).wait_send()

            for h in range(2):
                for core in range(CORES):
                    arrives = differs(h * half_size + home, first + core)

                    @pl.when(jnp.logical_and(arrives, (spot > 0) == far))
                    def _():
                        out_arrival(h, core, start, count).wait_recv()


def in_one_kernel(n, rngs, image, interp_weights, range_taps, range_shifts):
    width = image.shape[3]
    block = 2 * width // n
    tiles = block // LANES
    rows = LANES + 2 * HALO
    parts = len(tile_parts(tiles))
    rows_table, cols_table = phase_tables()
    vmem = pl.BlockSpec(memory_space=pltpu.VMEM)
    hbm = pl.BlockSpec(memory_space=pl.ANY)
    dma = pltpu.SemaphoreType.DMA
    f32, bf16 = jnp.float32, jnp.bfloat16
    return pl.pallas_call(
        functools.partial(merge_kernel, n, rngs),
        out_shape=pltpu.VMEM(image.shape, bf16),
        in_specs=[hbm] * 6,
        out_specs=vmem,
        scratch_shapes=[
            pltpu.VMEM(image.shape, bf16),
            pltpu.VMEM(interp_weights.shape, bf16),
            pltpu.SMEM(range_taps.shape, f32),
            pltpu.VMEM(range_shifts.shape, jnp.int32),
            pltpu.VMEM(rows_table.shape, f32),
            pltpu.VMEM(cols_table.shape, f32),
            dma((9,)),
            pltpu.VMEM((n, 2, ANGLES, block), bf16),
            pltpu.VMEM((n, 2, block + 2 * HALO + 8, ANGLES), f32),
            pltpu.VMEM((n, 2, HALO, ANGLES), bf16),
            pltpu.VMEM((n, 2, HALO, ANGLES), bf16),
            pltpu.VMEM((LEVELS, 4 * ANGLES, 4 * ANGLES), bf16),
            pltpu.VMEM((LEVELS - 1, 2, 2, rows, ANGLES), f32),
            pltpu.VMEM((n, 2, rows + 8, ANGLES), f32),
            pltpu.VMEM((4, rows + 8, ANGLES), f32),
            pltpu.VMEM((4, rows + 8, ANGLES), f32),
            pltpu.VMEM((4, rows + 8, ANGLES), f32),
            pltpu.VMEM((n // 2 * rows, 4 * ANGLES), bf16),
            pltpu.VMEM((n, 2, ANGLES, block), bf16),
            dma((2, CORES, parts)),
            dma((n, parts)),
            dma(()),
            dma(()),
            dma((tiles, n)),
            dma((2, CORES, tiles)),
            dma(()),
            dma(()),
            pltpu.SemaphoreType.REGULAR((n,)),
            pltpu.SemaphoreType.REGULAR,
        ],
        compiler_params=pltpu.CompilerParams(has_side_effects=True, collective_id=0),
    )(image, interp_weights, range_taps, range_shifts, rows_table, cols_table)


def fits_kernel(mesh, image_shape):
    n = mesh.shape["sub"]
    paired = mesh.shape["rng"] % CORES == 0
    tiled = image_shape[3] % (CORES * LANES) == 0 and image_shape[3] > CORES * LANES
    return paired and n == 2 * CORES and image_shape[1] == 2 and tiled and ANGLES == LANES


def per_device(mesh, image, *rest):
    if fits_kernel(mesh, image.shape):
        return in_one_kernel(mesh.shape["sub"], mesh.shape["rng"], image, *rest)
    return on_device(image, *rest)


def solution(mesh):
    return jax.shard_map(
        functools.partial(per_device, mesh),
        mesh=mesh,
        in_specs=(P(None, ("img", "sub"), None, "rng"), P(), P(), P()),
        out_specs=P(None, ("img", "sub"), None, "rng"),
        check_vma=False,
    )
```
